32 devices in a mesh: curve: 16 (over z, y, x), group: 2 (over core).
Axes of the slice: x: 2, y: 2, z: 4, core: 2. Of those that a mesh axis runs over, the one named last changes fastest.
Arguments:
- particles: float32 [512, 9, 128], P(('curve', 'group')), may hold values from -2 to 8, as said below
- counts: int32 [512], P(('curve', 'group')), may hold values from 16 to 128
- pair_lists: int32 [512, 13], P(('curve', 'group')), may hold values from -1 to 511, as said below
Outputs:
- density: float32 [512, 128], P(('curve', 'group'))
- acceleration: float32 [512, 3, 128], P(('curve', 'group'))
The draws below stay inside these ranges and needn't reach their ends.
Inputs may be any that keep to these rules, and one draw needn't show every extreme that they name: `particles`: the position of every slot of a cell lies in that cell's own unit box of the grid; channels 6, 7 and 8 are positive in every slot. `pair_lists`: the entries of row i other than -1 are distinct cells among i - 8 * 8 + 1 to i + 2 * 8 * 8 - 1, none equal to i, and no cell is named twice in one column.
All inputs are finite; a program needn't handle non-finite values.
Results may differ from the reference program's by a relative error of at most 0.0003.
Values sent between devices are 32-bit elements; how exact they have to be, the bound alone decides.
No kernel may reach another device: no remote copies, remote signals or barrier semaphores. Data moves between devices by JAX's collectives and lax.ppermute only.
A program may use at most 128 MiB of HBM per device.

```python
import math
import jax
import jax.numpy as jnp
from jax import lax

SLOTS = 128
SIDE = 8
PAIRS = 13
CELLS = 512


half_steps = [(-1, -1, 1), (0, -1, 1), (1, -1, 1), (-1, 0, 1), (0, 0, 1), (1, 0, 1), (-1, 1, 1), (0, 1, 1), (1, 1, 1), (-1, 1, 0), (0, 1, 0), (1, 1, 0), (1, 0, 0)]


def hilbert_place(rank, side_cells):
    across = jnp.zeros_like(rank)
    down = jnp.zeros_like(rank)
    remain = rank
    extent = 1
    while extent < side_cells:
        turn_x = remain // 2 % 2
        turn_y = (remain + turn_x) % 2
        flipped = (turn_y == 0) & (turn_x == 1)
        across = jnp.where(flipped, extent - 1 - across, across)
        down = jnp.where(flipped, extent - 1 - down, down)
        swapped = turn_y == 0
        across, down = (jnp.where(swapped, down, across), jnp.where(swapped, across, down))
        across = across + extent * turn_x
        down = down + extent * turn_y
        remain = remain // 4
        extent = extent * 2
    return (across, down)


def curve_cells(key):
    plane_size = SIDE * SIDE
    index = jnp.arange(CELLS, dtype=jnp.int32)
    layer = index // plane_size
    rank = index % plane_size
    rank = jnp.where(layer % 2 == 1, plane_size - 1 - rank, rank)
    across, down = hilbert_place(rank, SIDE)
    symmetry = jax.random.randint(jax.random.fold_in(key, 5), (CELLS // plane_size,), 0, 8)[layer]
    across = jnp.where(symmetry % 2 == 1, SIDE - 1 - across, across)
    down = jnp.where(symmetry // 2 % 2 == 1, SIDE - 1 - down, down)
    swapped = symmetry >= 4
    return (jnp.where(swapped, down, across), jnp.where(swapped, across, down), layer)


def draw_pair_lists(key, part):
    across, down, layer = curve_cells(key)
    layers = CELLS // (SIDE * SIDE)
    linear = (layer * SIDE + down) * SIDE + across
    lookup = jnp.zeros((CELLS,), jnp.int32).at[linear].set(jnp.arange(CELLS, dtype=jnp.int32))
    retain = jax.random.randint(jax.random.fold_in(key, 7), (CELLS, PAIRS), 0, 4) > 0
    columns = []
    for column, (step_x, step_y, step_z) in enumerate(half_steps):
        near_x = across + step_x
        near_y = down + step_y
        near_z = layer + step_z
        inside = (near_x >= 0) & (near_x < SIDE) & (near_y >= 0) & (near_y < SIDE) & (near_z < layers)
        if abs(step_x) + abs(step_y) + abs(step_z) == 3:
            inside = inside & retain[:, column]
        place = jnp.clip((near_z * SIDE + near_y) * SIDE + near_x, 0, CELLS - 1)
        columns.append(jnp.where(inside, lookup[place], -1))
    return jnp.stack(columns, axis=1).astype(jnp.int32)


def draw_particles(key, part):
    across, down, layer = curve_cells(key)
    corner = jnp.stack([across, down, layer], axis=1).astype(jnp.float32)[:, :, None]
    keys = jax.random.split(jax.random.fold_in(key, 23), 6)
    fraction = jax.random.uniform(keys[0], (CELLS, 3, SLOTS), jnp.float32, 0.0, 1.0)
    noise = jax.random.normal(keys[1], (CELLS, 3, SLOTS), jnp.float32)
    velocity = jnp.clip(0.5 * noise, -2.0, 2.0)
    position = corner + 0.999 * fraction
    smooth = jnp.exp(jax.random.uniform(keys[3], (CELLS, 1, SLOTS), jnp.float32, math.log(0.35), math.log(0.7)))
    masses = jnp.exp(jax.random.uniform(keys[4], (CELLS, 1, SLOTS), jnp.float32, math.log(0.007), math.log(0.028)))
    entropy = jnp.exp(jax.random.uniform(keys[5], (CELLS, 1, SLOTS), jnp.float32, 0.0, math.log(4.0)))
    return jnp.concatenate([position, velocity, smooth, masses, entropy], axis=1)


def with_ends(array, key, low, high):
    longest = array.shape.index(max(array.shape))
    spots = []
    for shift in (0, 1):
        where = [jax.random.randint(jax.random.fold_in(key, axis), (), 0, length) for axis, length in enumerate(array.shape)]
        where[longest] = (where[longest] + shift) % array.shape[longest]
        spots.append(tuple(where))
    return array.at[spots[0]].set(low).at[spots[1]].set(high)


def setup_inputs(seed: int = 0) -> dict:
    arg_keys = jax.random.split(jax.random.key(seed), 4)
    particles = draw_particles(jax.random.fold_in(arg_keys[3], 71), 0)
    counts = with_ends(jax.random.randint(arg_keys[1], (CELLS,), SLOTS // 8, SLOTS + 1), jax.random.fold_in(arg_keys[1], 1), SLOTS // 8, SLOTS).astype(jnp.int32)
    pair_lists = draw_pair_lists(jax.random.fold_in(arg_keys[3], 71), 0)
    return {"particles": particles, "counts": counts, "pair_lists": pair_lists}


gamma_index = 5.0 / 3.0
viscosity_alpha = 1.0
kernel_norm = 21.0 / (2.0 * 3.141592653589793)
slope_norm = 105.0 / (2.0 * 3.141592653589793)

def kernel_value(squared, smooth):
    scaled = jnp.sqrt(squared) / smooth
    remain = jnp.maximum(1.0 - 0.5 * scaled, 0.0)
    return kernel_norm / (smooth * smooth * smooth) * remain ** 4 * (1.0 + 2.0 * scaled)

def kernel_slope(squared, smooth):
    scaled = jnp.sqrt(squared) / smooth
    remain = jnp.maximum(1.0 - 0.5 * scaled, 0.0)
    return -slope_norm / smooth ** 5 * remain ** 3

def density_tile(target, source):
    offset = target[:, 0:3, :, None] - source[:, 0:3, None, :]
    squared = lax.optimization_barrier(jnp.sum(offset * offset, axis=1))
    to_target = lax.optimization_barrier(jnp.sum(kernel_value(squared, target[:, 6, :, None]) * source[:, 7, None, :], axis=2))
    to_source = lax.optimization_barrier(jnp.sum(kernel_value(squared, source[:, 6, None, :]) * target[:, 7, :, None], axis=1))
    return (to_target, to_source)

def force_tile(target, source):
    offset = target[:, 0:3, :, None] - source[:, 0:3, None, :]
    squared = lax.optimization_barrier(jnp.sum(offset * offset, axis=1))
    smooth_target = target[:, 6, :, None]
    smooth_source = source[:, 6, None, :]
    slope_target = kernel_slope(squared, smooth_target)
    slope_source = kernel_slope(squared, smooth_source)
    closing = lax.optimization_barrier(jnp.sum((target[:, 3:6, :, None] - source[:, 3:6, None, :]) * offset, axis=1))
    mean_smooth = 0.5 * (smooth_target + smooth_source)
    approach = jnp.minimum(mean_smooth * closing / (squared + 0.01 * mean_smooth * mean_smooth), 0.0)
    mean_sound = 0.5 * (target[:, 11, :, None] + source[:, 11, None, :])
    mean_density = 0.5 * (target[:, 9, :, None] + source[:, 9, None, :])
    viscous = viscosity_alpha * (2.0 * approach * approach - mean_sound * approach) / mean_density
    coupling = target[:, 10, :, None] * slope_target + source[:, 10, None, :] * slope_source + 0.5 * viscous * (slope_target + slope_source)
    to_target = -lax.optimization_barrier(jnp.sum(coupling[:, None] * source[:, 7, None, None, :] * offset, axis=3))
    to_source = lax.optimization_barrier(jnp.sum(coupling[:, None] * target[:, 7, None, :, None] * offset, axis=2))
    return (to_target, to_source)

def prepare(particles, counts):
    slot_count = particles.shape[2]
    occupied = (jnp.arange(slot_count, dtype=jnp.int32)[None, :] < counts[:, None]).astype(particles.dtype)
    masses = particles[:, 7] * occupied
    record = jnp.concatenate([particles[:, :7], masses[:, None], particles[:, 8:]], axis=1)
    return (record, occupied)

def secure(record):
    smooth = jnp.where(record[:, 7] > 0, record[:, 6], 1.0)
    return jnp.concatenate([record[:, :6], smooth[:, None], record[:, 7:]], axis=1)

def thermal(record, density):
    bounded = jnp.where(record[:, 7] > 0, density, 1.0)
    pressure_term = record[:, 8] * bounded ** (gamma_index - 2.0)
    sound = jnp.sqrt(gamma_index * record[:, 8] * bounded ** (gamma_index - 1.0))
    return jnp.concatenate([record, bounded[:, None], pressure_term[:, None], sound[:, None]], axis=1)

def sweep_pairs(augmented, partner, weights, tile, inner_shape):
    total_cells = augmented.shape[0]
    slot_count = augmented.shape[2]
    pair_count = partner.shape[1]
    block_cells = [size for size in (16, 8) if total_cells % size == 0][0]
    summed = jnp.zeros((total_cells,) + inner_shape + (slot_count,), augmented.dtype)

    def advance(block_index, summed):
        leading = block_index * block_cells
        target = lax.dynamic_slice_in_dim(augmented, leading, block_cells, 0)
        sources = lax.dynamic_slice_in_dim(partner, leading, block_cells, 0).reshape(-1)
        factor = lax.dynamic_slice_in_dim(weights, leading, block_cells, 0).reshape((-1,) + (1,) * (len(inner_shape) + 1))
        source = jnp.take(augmented, sources, axis=0)
        paired = jnp.repeat(target, pair_count, axis=0)
        to_target, to_source = tile(paired, source)
        inside = tile(target, target)[0]
        gathered = (to_target * factor).reshape((block_cells, pair_count) + inner_shape + (slot_count,)).sum(axis=1)
        current = lax.dynamic_slice_in_dim(summed, leading, block_cells, 0)
        summed = lax.dynamic_update_slice_in_dim(summed, current + inside + gathered, leading, 0)
        return summed.at[sources].add(to_source * factor)
    return lax.fori_loop(0, total_cells // block_cells, advance, summed)

def reference(particles, counts, pair_lists):
    total_cells = particles.shape[0]
    record, occupied = prepare(particles, counts)
    record = secure(record)
    usable = pair_lists >= 0
    own_index = jnp.arange(total_cells, dtype=jnp.int32)[:, None]
    partner = jnp.where(usable, pair_lists, own_index).astype(jnp.int32)
    weights = usable.astype(record.dtype)
    density = sweep_pairs(record, partner, weights, density_tile, ())
    augmented = thermal(record, density)
    acceleration = sweep_pairs(augmented, partner, weights, force_tile, (3,))
    return (density * occupied, acceleration * occupied[:, None])
```

```python
import jax
import jax.numpy as jnp
from jax import lax
from jax.experimental import pallas as pl
from jax.experimental.pallas import tpu as pltpu
from jax.sharding import PartitionSpec as P


FARTHEST = 127

gamma_index = 5.0 / 3.0
kernel_norm = 21.0 / (2.0 * 3.141592653589793)
slope_norm = 105.0 / (2.0 * 3.141592653589793)

LANES = 128
DENSITY_ROWS, DENSITY_TILES = 16, 4
FORCE_ROWS, FORCE_TILES = 16, 4
TINY = 1.2e-38
AXES = ("curve", "group")


def swap_cores(block):
    return lax.ppermute(block, "group", [(0, 1), (1, 0)])


def reach_of(local_cells):
    return -(-FARTHEST // (2 * local_cells))


def surround(block):
    chips = lax.axis_size("curve")
    chip_block = jnp.concatenate([block, swap_cores(block)], axis=0)
    fetched = []
    for k in range(1, reach_of(block.shape[0]) + 1):
        route = []
        for chip in range(chips):
            route.append((2 * ((chip + k) % chips), 2 * chip))
            route.append((2 * ((chip - k) % chips) + 1, 2 * chip + 1))
        fetched.append(lax.ppermute(chip_block, AXES, route))
    fetched = jnp.concatenate(fetched, axis=0)
    return jnp.concatenate([chip_block, fetched, swap_cores(fetched)], axis=0)


def window_ids(local_cells):
    chip, core = lax.axis_index("curve"), lax.axis_index("group")
    side = 1 - 2 * core
    inner = jnp.arange(local_cells, dtype=jnp.int32)
    mine = jnp.concatenate([core * local_cells + inner, (1 - core) * local_cells + inner])
    other = jnp.concatenate([(1 - core) * local_cells + inner, core * local_cells + inner])
    reach = reach_of(local_cells)
    pieces = [chip * 2 * local_cells + mine]
    pieces += [(chip + side * k) * 2 * local_cells + mine for k in range(1, reach + 1)]
    pieces += [(chip - side * k) * 2 * local_cells + other for k in range(1, reach + 1)]
    return jnp.concatenate(pieces)


def pack_sources(cell, ahead_ref, behind_ref, columns, tables, packs, pad_tiles):
    lane = lax.broadcasted_iota(jnp.int32, (1, LANES), 1)
    held = [jnp.zeros(pack.shape[1:], jnp.float32) for pack in packs]
    place = jnp.int32(0)
    for entry in range(2 * columns + 1):
        if entry <= columns:
            code = ahead_ref[cell * LANES + entry]
        else:
            code = behind_ref[cell * LANES + entry - columns - 1]
        row = lax.shift_right_logical(code, 8)
        count = lax.bitwise_and(code, 255)
        tile = lax.shift_right_logical(place, 7)
        turn = lax.bitwise_and(place, 127)
        place = place + count
        crossed = lax.shift_right_logical(place, 7) > tile
        beyond = lane >= turn
        for n, (table, pack) in enumerate(zip(tables, packs)):
            rolled = pltpu.roll(table[row], turn, 1)
            merged = jnp.where(beyond, rolled, held[n])
            pack[tile] = merged
            held[n] = jnp.where(crossed, rolled, merged)
    tile = lax.shift_right_logical(place, 7)
    inside = lane < lax.bitwise_and(place, 127)
    for n, pack in enumerate(packs):
        pack[tile] = jnp.where(inside, held[n], 0.0)
        for extra in range(1, pad_tiles):
            pack[tile + extra] = jnp.zeros(pack.shape[1:], jnp.float32)
    return lax.shift_right_logical(place + 127, 7)


def density_kernel(ahead_ref, behind_ref, table_ref, own_ref, out_ref, pack_ref, spread_ref, sums_ref, *, columns):
    local_cells = own_ref.shape[0]
    rows, tiles = DENSITY_ROWS, DENSITY_TILES
    sums_ref[...] = jnp.zeros(sums_ref.shape, jnp.float32)

    def per_cell(cell, carry):
        tile_count = pack_sources(cell, ahead_ref, behind_ref, columns, [table_ref], [pack_ref], tiles)
        target = jnp.transpose(own_ref[cell])
        for c in range(4):
            spread_ref[c] = jnp.broadcast_to(target[:, c : c + 1], (LANES, LANES))
        count = lax.bitwise_and(ahead_ref[cell * LANES + columns], 255)

        def per_rows(group, carry):
            span = pl.ds(pl.multiple_of(group * rows, rows), rows)
            xa, ya, za, ia = (spread_ref[c, span, :] for c in range(4))

            def per_tiles(step, total):
                for u in range(tiles):
                    at = step * tiles + u
                    dx = xa - pack_ref[at, 0:1, :]
                    dy = ya - pack_ref[at, 1:2, :]
                    dz = za - pack_ref[at, 2:3, :]
                    squared = dx * dx + dy * dy + dz * dz
                    scaled = squared * lax.rsqrt(jnp.maximum(squared, TINY)) * ia
                    remain = jnp.maximum(4.0 - scaled, 0.0)
                    remain = remain * remain
                    total = total + remain * remain * ((1.0 + scaled) * pack_ref[at, 3:4, :])
                return total

            sums_ref[cell, span, :] = lax.fori_loop(
                0, (tile_count + tiles - 1) // tiles, per_tiles, jnp.zeros((rows, LANES), jnp.float32)
            )
            return carry

        return lax.fori_loop(0, (count + rows - 1) // rows, per_rows, carry)

    lax.fori_loop(0, local_cells, per_cell, 0)
    lane = lax.broadcasted_iota(jnp.int32, (LANES, LANES), 1)
    columns_of = jnp.zeros((LANES, LANES), jnp.float32)
    for cell in range(local_cells):
        columns_of = jnp.where(lane == cell, jnp.sum(sums_ref[cell], axis=1, keepdims=True), columns_of)
    out_ref[...] = jnp.transpose(columns_of)[:local_cells]


def force_kernel(
    ahead_ref, behind_ref, table_ref, state_ref, out_ref, pack_ref, state_pack_ref, spread_ref, sums_ref, *, columns
):
    local_cells = out_ref.shape[1]
    rows, tiles = FORCE_ROWS, FORCE_TILES
    sums_ref[...] = jnp.zeros(sums_ref.shape, jnp.float32)

    def per_cell(cell, carry):
        tile_count = pack_sources(
            cell, ahead_ref, behind_ref, columns, [table_ref, state_ref], [pack_ref, state_pack_ref], tiles
        )
        target = jnp.transpose(table_ref[cell])
        state = jnp.transpose(state_ref[cell])
        for n, c in enumerate((0, 1, 2, 4, 5, 6)):
            spread_ref[n] = jnp.broadcast_to(target[:, c : c + 1], (LANES, LANES))
        for c in range(6):
            spread_ref[6 + c] = jnp.broadcast_to(state[:, c : c + 1], (LANES, LANES))
        count = lax.bitwise_and(ahead_ref[cell * LANES + columns], 255)

        def per_rows(group, carry):
            span = pl.ds(pl.multiple_of(group * rows, rows), rows)

            def per_tiles(step, total):
                for u in range(tiles):
                    at = step * tiles + u
                    xa, ya, za, ua, va, wa, ra, fa, ca, ga, sa, ja = (spread_ref[c, span, :] for c in range(12))
                    dx = xa - pack_ref[at, 0:1, :]
                    dy = ya - pack_ref[at, 1:2, :]
                    dz = za - pack_ref[at, 2:3, :]
                    squared = dx * dx + dy * dy + dz * dz
                    apart = squared * lax.rsqrt(jnp.maximum(squared, TINY))
                    closing = (
                        (ua - pack_ref[at, 4:5, :]) * dx
                        + (va - pack_ref[at, 5:6, :]) * dy
                        + (wa - pack_ref[at, 6:7, :]) * dz
                    )
                    slope_a = jnp.maximum(sa - apart * ja, 0.0)
                    slope_a = slope_a * slope_a * slope_a
                    slope_b = jnp.maximum(state_pack_ref[at, 4:5, :] - apart * state_pack_ref[at, 5:6, :], 0.0)
                    slope_b = slope_b * slope_b * slope_b
                    width = ga + state_pack_ref[at, 3:4, :]
                    approach = jnp.minimum(width * closing, 0.0) / (squared + width * width)
                    viscous = (
                        approach
                        * (approach - (ca + state_pack_ref[at, 2:3, :]))
                        / (ra + state_pack_ref[at, 0:1, :])
                    )
                    coupling = (
                        (fa + viscous) * slope_a + (state_pack_ref[at, 1:2, :] + viscous) * slope_b
                    ) * pack_ref[at, 3:4, :]
                    total = (total[0] + coupling * dx, total[1] + coupling * dy, total[2] + coupling * dz)
                return total

            empty = jnp.zeros((rows, LANES), jnp.float32)
            total = lax.fori_loop(0, (tile_count + tiles - 1) // tiles, per_tiles, (empty, empty, empty))
            for d in range(3):
                sums_ref[d, cell, span, :] = total[d]
            return carry

        return lax.fori_loop(0, (count + rows - 1) // rows, per_rows, carry)

    lax.fori_loop(0, local_cells, per_cell, 0)
    lane = lax.broadcasted_iota(jnp.int32, (LANES, LANES), 1)
    for d in range(3):
        columns_of = jnp.zeros((LANES, LANES), jnp.float32)
        for cell in range(local_cells):
            columns_of = jnp.where(lane == cell, jnp.sum(sums_ref[d, cell], axis=1, keepdims=True), columns_of)
        out_ref[d] = jnp.transpose(columns_of)[:local_cells]


def partner_codes(window_lists, pair_lists, ids, local_cells):
    columns = pair_lists.shape[1]
    listed = lax.shift_right_logical(window_lists, 8) - 1
    held = lax.bitwise_and(window_lists, 255)
    code = jnp.arange(ids.shape[0], dtype=jnp.int32)[:, None] * 256 + held
    own = ids[:local_cells]
    wanted = jnp.where(pair_lists >= 0, pair_lists, -(1 << 30))
    wanted = jnp.concatenate(
        [wanted, own[:, None], jnp.full((local_cells, LANES - columns - 1), -(1 << 30), jnp.int32)], axis=1
    )
    ahead = jnp.max(jnp.where(ids[:, None, None] == wanted[None], code[:, None, :], 0), axis=0)
    behind = jnp.max(jnp.where(listed[:, None, :] == own[None, :, None], code[:, None, :], 0), axis=0)
    return ahead.reshape(-1), behind.reshape(-1)


def per_device(particles, counts, pair_lists):
    local_cells, _, slots = particles.shape
    columns = pair_lists.shape[1]
    assert slots == LANES
    occupied = (jnp.arange(slots, dtype=jnp.int32)[None, :] < counts[:, None]).astype(jnp.float32)
    masses = particles[:, 7] * occupied
    smooth = jnp.where(masses > 0, particles[:, 6], 1.0)
    lists = jnp.concatenate(
        [pair_lists + 1, jnp.zeros((local_cells, slots - columns), jnp.int32)], axis=1
    ) * 256 + counts[:, None]
    sent = jnp.concatenate(
        [particles[:, 0:3], masses[:, None], particles[:, 3:6], lists.astype(jnp.float32)[:, None]], axis=1
    )
    table = surround(sent)
    ids = window_ids(local_cells)
    ahead, behind = partner_codes(table[:, 7].astype(jnp.int32), pair_lists, ids, local_cells)
    own = jnp.concatenate(
        [particles[:, 0:3], (2.0 / smooth)[:, None], jnp.zeros((local_cells, 4, slots), jnp.float32)], axis=1
    )
    most_tiles = 2 * columns + 2
    scalars = pl.BlockSpec(memory_space=pltpu.SMEM)
    whole = pl.BlockSpec(memory_space=pltpu.VMEM)
    raw = pl.pallas_call(
        lambda *refs: density_kernel(*refs, columns=columns),
        out_shape=jax.ShapeDtypeStruct((local_cells, slots), jnp.float32),
        in_specs=[scalars, scalars, whole, whole],
        out_specs=whole,
        scratch_shapes=[
            pltpu.VMEM((most_tiles + DENSITY_TILES, 8, LANES), jnp.float32),
            pltpu.VMEM((4, LANES, LANES), jnp.float32),
            pltpu.VMEM((local_cells, LANES, LANES), jnp.float32),
        ],
        name="density_sweep",
    )(ahead, behind, table, own)
    density = raw * (kernel_norm / 256.0) / (smooth * smooth * smooth) * occupied
    bounded = jnp.where(masses > 0, density, 1.0)
    pressure_term = particles[:, 8] * bounded ** (gamma_index - 2.0)
    sound = jnp.sqrt(gamma_index * particles[:, 8] * bounded ** (gamma_index - 1.0))
    steep = (slope_norm / smooth**5) ** (1.0 / 3.0)
    state = jnp.stack(
        [
            bounded * 0.005,
            pressure_term,
            sound * 0.025,
            smooth * 0.05,
            steep,
            steep * (0.5 / smooth),
            jnp.zeros_like(smooth),
            jnp.zeros_like(smooth),
        ],
        axis=1,
    )
    states = surround(state)
    moved = pl.pallas_call(
        lambda *refs: force_kernel(*refs, columns=columns),
        out_shape=jax.ShapeDtypeStruct((3, local_cells, slots), jnp.float32),
        in_specs=[scalars, scalars, whole, whole],
        out_specs=whole,
        scratch_shapes=[
            pltpu.VMEM((most_tiles + FORCE_TILES, 8, LANES), jnp.float32),
            pltpu.VMEM((most_tiles + FORCE_TILES, 8, LANES), jnp.float32),
            pltpu.VMEM((12, LANES, LANES), jnp.float32),
            pltpu.VMEM((3, local_cells, LANES, LANES), jnp.float32),
        ],
        name="force_sweep",
    )(ahead, behind, table, states)
    acceleration = jnp.transpose(moved, (1, 0, 2)) * occupied[:, None]
    return density, acceleration


def solution(mesh):
    in_specs = (P(AXES, None, None), P(AXES), P(AXES, None))
    out_specs = (P(AXES, None), P(AXES, None, None))
    return jax.shard_map(per_device, mesh=mesh, in_specs=in_specs, out_specs=out_specs, check_vma=False)
```

```python
import jax
import jax.numpy as jnp
from jax import lax
from jax.experimental import pallas as pl
from jax.experimental.pallas import tpu as pltpu
from jax.sharding import PartitionSpec as P


FARTHEST = 127

gamma_index = 5.0 / 3.0
kernel_norm = 21.0 / (2.0 * 3.141592653589793)
slope_norm = 105.0 / (2.0 * 3.141592653589793)

LANES = 128
TINY = 1.2e-38
AXES = ("curve", "group")


def swap_cores(block):
    return lax.ppermute(block, "group", [(0, 1), (1, 0)])


def reach_of(local_cells):
    return -(-FARTHEST // (2 * local_cells))


def route_of(chips, k):
    route = []
    for chip in range(chips):
        route.append((2 * (chip + k) if chip + k < chips else 2 * chip + 1, 2 * chip))
        route.append((2 * (chip - k) + 1 if chip - k >= 0 else 2 * chip, 2 * chip + 1))
    return route


def surround(block):
    chips = lax.axis_size("curve")
    chip_block = jnp.concatenate([block, swap_cores(block)], axis=0)
    reach = reach_of(block.shape[0])
    fetched = [lax.ppermute(chip_block, AXES, route_of(chips, k)) for k in range(1, reach + 1)]
    fetched = jnp.concatenate(fetched, axis=0)
    return jnp.concatenate([chip_block, fetched, swap_cores(fetched)], axis=0)


def window_ids(local_cells):
    chip, core = lax.axis_index("curve"), lax.axis_index("group")
    side = 1 - 2 * core
    inner = jnp.arange(local_cells, dtype=jnp.int32)
    mine = jnp.concatenate([core * local_cells + inner, (1 - core) * local_cells + inner])
    other = jnp.concatenate([(1 - core) * local_cells + inner, core * local_cells + inner])
    reach = reach_of(local_cells)
    pieces = [chip * 2 * local_cells + mine]
    pieces += [(chip + side * k) * 2 * local_cells + mine for k in range(1, reach + 1)]
    pieces += [(chip - side * k) * 2 * local_cells + other for k in range(1, reach + 1)]
    return jnp.concatenate(pieces)


def pack_sources(cell, ahead_ref, behind_ref, columns, tables, packs, pad_tiles):
    lane = lax.broadcasted_iota(jnp.int32, (1, LANES), 1)
    held = [jnp.zeros(pack.shape[1:], jnp.float32) for pack in packs]
    place = jnp.int32(0)
    for entry in range(2 * columns + 1):
        if entry <= columns:
            code = ahead_ref[cell * LANES + entry]
        else:
            code = behind_ref[cell * LANES + entry - columns - 1]
        row = lax.shift_right_logical(code, 8)
        count = lax.bitwise_and(code, 255)
        tile = lax.shift_right_logical(place, 7)
        turn = lax.bitwise_and(place, 127)
        place = place + count
        crossed = lax.shift_right_logical(place, 7) > tile
        beyond = lane >= turn
        for n, (table, pack) in enumerate(zip(tables, packs)):
            rolled = pltpu.roll(table[row], turn, 1)
            merged = jnp.where(beyond, rolled, held[n])
            pack[tile] = merged
            held[n] = jnp.where(crossed, rolled, merged)
    tile = lax.shift_right_logical(place, 7)
    inside = lane < lax.bitwise_and(place, 127)
    for n, pack in enumerate(packs):
        pack[tile] = jnp.where(inside, held[n], 0.0)
        for extra in range(1, pad_tiles):
            pack[tile + extra] = jnp.zeros(pack.shape[1:], jnp.float32)
    return lax.shift_right_logical(place + 127, 7)


def each_cell(local_cells, prepare, sweep):
    def per_pair(pair, carry):
        tile_counts = [prepare(2 * pair + n, n) for n in range(2)]
        for n in range(2):
            sweep(2 * pair + n, n, tile_counts[n])
        return carry

    lax.fori_loop(0, local_cells // 2, per_pair, 0)


def each_group(count, tile_count, body, finish, zeros):
    fours = lax.shift_right_logical(tile_count + 1, 2)
    twos = jnp.where(tile_count > 4 * fours, 1, 0)

    def per_group(start, rows):
        span = pl.ds(pl.multiple_of(start, 8), rows)
        step = body(span)
        total = zeros(rows)
        total = lax.fori_loop(0, fours, lambda k, t: step(4 * k, 4, t), total)
        total = lax.fori_loop(0, twos, lambda k, t: step(4 * fours, 2, t), total)
        finish(span, total)

    def whole(group, carry):
        per_group(group * 16, 16)
        return carry

    eights = lax.shift_right_logical(count + 7, 3)
    wholes = lax.shift_right_logical(eights, 1)
    lax.fori_loop(0, wholes, whole, 0)

    def rest(_, carry):
        per_group(wholes * 16, 8)
        return carry

    lax.fori_loop(0, lax.bitwise_and(eights, 1), rest, 0)


def row_sums(sums, local_cells):
    lane = lax.broadcasted_iota(jnp.int32, (LANES, LANES), 1)
    held = jnp.zeros((LANES, LANES), jnp.float32)
    for cell in range(local_cells):
        held = jnp.where(lane == cell, jnp.sum(sums[cell], axis=1, keepdims=True), held)
    return jnp.transpose(held)[:local_cells]


def prepare_kernel(counts_ref, particles_ref, lists_ref, sent_ref, padded_ref):
    local_cells, columns = lists_ref.shape
    lane = lax.broadcasted_iota(jnp.int32, (1, LANES), 1)
    padded_ref[...] = jnp.full(padded_ref.shape, -1, jnp.int32)
    padded_ref[:, 0:columns] = lists_ref[...]
    for cell in range(local_cells):
        count = counts_ref[cell]
        row = slice(cell, cell + 1)
        for c, d in enumerate((0, 1, 2, None, 3, 4, 5)):
            if d is not None:
                sent_ref[cell, c : c + 1, :] = particles_ref[d, row, :]
        sent_ref[cell, 3:4, :] = jnp.where(lane < count, particles_ref[7, row, :], 0.0)
        sent_ref[cell, 7:8, :] = ((padded_ref[row, :] + 1) * 256 + count).astype(jnp.float32)


def density_kernel(
    counts_ref, ahead_ref, behind_ref, table_ref, particles_ref, out_ref, state_ref, pack_ref, spread_ref, sums_ref,
    widths_ref, *, columns,
):
    local_cells = particles_ref.shape[1]
    widths_ref[0:local_cells, :] = 2.0 / particles_ref[6]
    for cell in range(local_cells):
        state_ref[cell, 0:3, :] = table_ref[cell, 0:3, :]
        state_ref[cell, 3:4, :] = widths_ref[cell : cell + 1, :]

    def prepare(cell, n):
        tile_count = pack_sources(cell, ahead_ref, behind_ref, columns, [table_ref], [pack_ref.at[n]], 2)
        target = jnp.transpose(state_ref[cell])
        for d in range(4):
            spread_ref[n, d] = jnp.broadcast_to(target[:, d : d + 1], (LANES, LANES))
        return tile_count

    def sweep(cell, n, tile_count):
        def body(span):
            xa, ya, za, ia = (spread_ref[n, c, span, :] for c in range(4))

            def step(first, tiles, total):
                for u in range(tiles):
                    at = first + u
                    dx = xa - pack_ref[n, at, 0:1, :]
                    dy = ya - pack_ref[n, at, 1:2, :]
                    dz = za - pack_ref[n, at, 2:3, :]
                    squared = dx * dx + dy * dy + dz * dz
                    scaled = squared * lax.rsqrt(jnp.maximum(squared, TINY)) * ia
                    remain = jnp.maximum(4.0 - scaled, 0.0)
                    remain = remain * remain
                    total = total + remain * remain * ((1.0 + scaled) * pack_ref[n, at, 3:4, :])
                return total

            return step

        def finish(span, total):
            sums_ref[cell, span, :] = total

        each_group(counts_ref[cell], tile_count, body, finish, lambda rows: jnp.zeros((rows, LANES), jnp.float32))

    each_cell(local_cells, prepare, sweep)
    raw = row_sums(sums_ref, local_cells)
    masses = jnp.concatenate([table_ref[cell, 3:4, :] for cell in range(local_cells)], axis=0)
    smooth, entropy = particles_ref[6], particles_ref[8]
    held = masses > 0.0
    smooth = jnp.where(held, smooth, 1.0)
    density = jnp.where(held, raw * (kernel_norm / 256.0) / (smooth * smooth * smooth), 0.0)
    out_ref[...] = density
    bounded = jnp.where(held, density, 1.0)
    log_density, log_smooth = jnp.log(bounded), jnp.log(smooth)
    pressure_term = entropy * jnp.exp((gamma_index - 2.0) * log_density)
    sound = jnp.sqrt(gamma_index * entropy * jnp.exp((gamma_index - 1.0) * log_density))
    steep = slope_norm ** (1.0 / 3.0) * jnp.exp((-5.0 / 3.0) * log_smooth)
    rows = (bounded * 0.005, pressure_term, sound * 0.025, smooth * 0.05, steep, steep * (0.5 / smooth))
    for cell in range(local_cells):
        for c, row in enumerate(rows):
            state_ref[cell, c : c + 1, :] = row[cell : cell + 1]
        state_ref[cell, 6:8, :] = jnp.zeros((2, LANES), jnp.float32)


def force_kernel(
    counts_ref, ahead_ref, behind_ref, table_ref, state_ref, out_ref, pack_ref, state_pack_ref, spread_ref, sums_ref,
    *, columns,
):
    local_cells = out_ref.shape[1]

    def prepare(cell, n):
        tile_count = pack_sources(
            cell, ahead_ref, behind_ref, columns, [table_ref, state_ref], [pack_ref.at[n], state_pack_ref.at[n]], 2
        )
        target = jnp.transpose(table_ref[cell])
        state = jnp.transpose(state_ref[cell])
        for c, d in enumerate((0, 1, 2, 4, 5, 6)):
            spread_ref[n, c] = jnp.broadcast_to(target[:, d : d + 1], (LANES, LANES))
        for c in range(6):
            spread_ref[n, 6 + c] = jnp.broadcast_to(state[:, c : c + 1], (LANES, LANES))
        return tile_count

    def sweep(cell, n, tile_count):
        def body(span):
            def step(first, tiles, total):
                for u in range(tiles):
                    at = first + u
                    xa, ya, za, ua, va, wa, ra, fa, ca, ga, sa, ja = (spread_ref[n, c, span, :] for c in range(12))
                    xb, yb, zb, mb, ub, vb, wb = (pack_ref[n, at, c : c + 1, :] for c in range(7))
                    rb, fb, cb, gb, sb, jb = (state_pack_ref[n, at, c : c + 1, :] for c in range(6))
                    dx, dy, dz = xa - xb, ya - yb, za - zb
                    squared = dx * dx + dy * dy + dz * dz
                    apart = squared * lax.rsqrt(jnp.maximum(squared, TINY))
                    closing = (ua - ub) * dx + (va - vb) * dy + (wa - wb) * dz
                    slope_a = jnp.maximum(sa - apart * ja, 0.0)
                    slope_a = slope_a * slope_a * slope_a
                    slope_b = jnp.maximum(sb - apart * jb, 0.0)
                    slope_b = slope_b * slope_b * slope_b
                    width = ga + gb
                    approach = jnp.minimum(width * closing, 0.0) / (squared + width * width)
                    viscous = approach * (approach - (ca + cb)) / (ra + rb)
                    coupling = ((fa + viscous) * slope_a + (fb + viscous) * slope_b) * mb
                    total = (total[0] + coupling * dx, total[1] + coupling * dy, total[2] + coupling * dz)
                return total

            return step

        def finish(span, total):
            for d in range(3):
                sums_ref[d, cell, span, :] = total[d]

        each_group(
            counts_ref[cell], tile_count, body, finish, lambda rows: (jnp.zeros((rows, LANES), jnp.float32),) * 3
        )

    each_cell(local_cells, prepare, sweep)
    held = jnp.concatenate([table_ref[cell, 3:4, :] for cell in range(local_cells)], axis=0) > 0.0
    for d in range(3):
        out_ref[d] = jnp.where(held, row_sums(sums_ref.at[d], local_cells), 0.0)


def partner_codes(window_lists, pair_lists, ids, local_cells):
    columns = pair_lists.shape[1]
    real = (ids >= 0) & (ids < lax.axis_size("curve") * 2 * local_cells)
    listed = jnp.where(real[:, None], lax.shift_right_logical(window_lists, 8) - 1, -1)
    held = lax.bitwise_and(window_lists, 255)
    code = jnp.arange(ids.shape[0], dtype=jnp.int32)[:, None] * 256 + held
    own = ids[:local_cells]
    wanted = jnp.where(pair_lists >= 0, pair_lists, -(1 << 30))
    wanted = jnp.concatenate(
        [wanted, own[:, None], jnp.full((local_cells, LANES - columns - 1), -(1 << 30), jnp.int32)], axis=1
    )
    ahead = jnp.max(jnp.where(ids[:, None, None] == wanted[None], code[:, None, :], 0), axis=0)
    behind = jnp.max(jnp.where(listed[:, None, :] == own[None, :, None], code[:, None, :], 0), axis=0)
    return ahead.reshape(-1), behind.reshape(-1)


def on_chip(array):
    return pltpu.with_memory_space_constraint(array, pltpu.VMEM)


def per_device(particles, counts, pair_lists):
    local_cells, channels, slots = particles.shape
    columns = pair_lists.shape[1]
    assert slots == LANES and local_cells % 2 == 0
    scalars = pl.BlockSpec(memory_space=pltpu.SMEM)
    whole = pl.BlockSpec(memory_space=pltpu.VMEM)
    floats = lambda *shape: pltpu.VMEM(shape, jnp.float32)
    particles = jnp.transpose(particles, (1, 0, 2))
    sent = pl.pallas_call(
        prepare_kernel,
        out_shape=jax.ShapeDtypeStruct((local_cells, 8, slots), jnp.float32),
        in_specs=[scalars, whole, whole],
        out_specs=whole,
        scratch_shapes=[pltpu.VMEM((local_cells, LANES), jnp.int32)],
        name="prepare",
    )(counts, particles, pair_lists)
    window = surround(sent)
    table = on_chip(window)
    ids = window_ids(local_cells)
    ahead, behind = partner_codes(window[:, 7].astype(jnp.int32), pair_lists, ids, local_cells)
    most_tiles = 2 * columns + 5
    density, state = pl.pallas_call(
        lambda *refs: density_kernel(*refs, columns=columns),
        out_shape=(
            jax.ShapeDtypeStruct((local_cells, slots), jnp.float32),
            jax.ShapeDtypeStruct((local_cells, 8, slots), jnp.float32),
        ),
        in_specs=[scalars, scalars, scalars, whole, whole],
        out_specs=(whole, whole),
        scratch_shapes=[
            floats(2, most_tiles, 8, LANES),
            floats(2, 4, LANES, LANES),
            floats(local_cells, LANES, LANES),
            floats(local_cells, LANES),
        ],
        name="density_sweep",
    )(counts, ahead, behind, table, particles)
    states = on_chip(surround(state))
    acceleration = pl.pallas_call(
        lambda *refs: force_kernel(*refs, columns=columns),
        out_shape=jax.ShapeDtypeStruct((3, local_cells, slots), jnp.float32),
        in_specs=[scalars, scalars, scalars, whole, whole],
        out_specs=whole,
        scratch_shapes=[
            floats(2, most_tiles, 8, LANES),
            floats(2, most_tiles, 8, LANES),
            floats(2, 12, LANES, LANES),
            floats(3, local_cells, LANES, LANES),
        ],
        name="force_sweep",
    )(counts, ahead, behind, table, states)
    return density, jnp.transpose(acceleration, (1, 0, 2))


def solution(mesh):
    in_specs = (P(AXES, None, None), P(AXES), P(AXES, None))
    out_specs = (P(AXES, None), P(AXES, None, None))
    return jax.shard_map(per_device, mesh=mesh, in_specs=in_specs, out_specs=out_specs, check_vma=False)
```

```python
import jax
import jax.numpy as jnp
from jax import lax
from jax.experimental import pallas as pl
from jax.experimental.pallas import tpu as pltpu
from jax.sharding import PartitionSpec as P


FARTHEST = 127

gamma_index = 5.0 / 3.0
kernel_norm = 21.0 / (2.0 * 3.141592653589793)
slope_norm = 105.0 / (2.0 * 3.141592653589793)

LANES = 128
ROOM = 12 << 20
TINY = 1.2e-38
AXES = ("curve", "group")


def swap_cores(block):
    return lax.ppermute(block, "group", [(0, 1), (1, 0)])


def reach_of(local_cells):
    return -(-FARTHEST // (2 * local_cells))


def route_of(chips, k):
    route = []
    for chip in range(chips):
        route.append((2 * (chip + k) if chip + k < chips else 2 * chip + 1, 2 * chip))
        route.append((2 * (chip - k) + 1 if chip - k >= 0 else 2 * chip, 2 * chip + 1))
    return route


def surround(block, beside):
    chips = lax.axis_size("curve")
    chip_block = jnp.concatenate([block, swap_cores(block)], axis=0)
    reach = reach_of(block.shape[0])
    fetched = []
    for k in range(1, reach + 1):
        fetched.append(lax.ppermute(chip_block, AXES, route_of(chips, k)))
    made = beside(chip_block)
    fetched = jnp.concatenate(fetched, axis=0)
    return jnp.concatenate([chip_block, fetched, swap_cores(fetched)], axis=0), made


def window_starts(chip, core, local_cells, reach):
    side = 1 - 2 * core
    runs = [(chip, core), (chip, 1 - core)]
    for k in range(1, reach + 1):
        runs += [(chip + side * k, core), (chip + side * k, 1 - core)]
    for k in range(1, reach + 1):
        runs += [(chip - side * k, 1 - core), (chip - side * k, core)]
    return [((2 * where + half) * local_cells, where) for where, half in runs]


def pack_sources(cell, codes_ref, columns, tables, packs, pad_tiles):
    lane = lax.broadcasted_iota(jnp.int32, (1, LANES), 1)
    held = [jnp.zeros(pack.shape[1:], jnp.float32) for pack in packs]
    place = jnp.int32(0)
    for entry in range(2 * columns + 1):
        code = codes_ref[cell, entry]
        row = lax.shift_right_logical(code, 8)
        count = lax.bitwise_and(code, 255)
        tile = lax.shift_right_logical(place, 7)
        turn = lax.bitwise_and(place, 127)
        place = place + count
        crossed = lax.shift_right_logical(place, 7) > tile
        beyond = lane >= turn
        for n, (table, pack) in enumerate(zip(tables, packs)):
            rolled = pltpu.roll(table[row], turn, 1)
            merged = jnp.where(beyond, rolled, held[n])
            pack[tile] = merged
            held[n] = jnp.where(crossed, rolled, merged)
    tile = lax.shift_right_logical(place, 7)
    inside = lane < lax.bitwise_and(place, 127)
    for n, pack in enumerate(packs):
        pack[tile] = jnp.where(inside, held[n], 0.0)
        for extra in range(1, pad_tiles):
            pack[tile + extra] = jnp.zeros(pack.shape[1:], jnp.float32)
    return lax.shift_right_logical(place + 127, 7)


def each_group(count, tile_count, body, finish, zeros):
    fours = lax.shift_right_logical(tile_count + 1, 2)
    twos = jnp.where(tile_count > 4 * fours, 1, 0)

    def per_group(start, rows):
        span = pl.ds(pl.multiple_of(start, 8), rows)
        step = body(span)
        total = zeros(rows)
        total = lax.fori_loop(0, fours, lambda k, t: step(4 * k, 4, t), total)
        total = lax.fori_loop(0, twos, lambda k, t: step(4 * fours, 2, t), total)
        finish(span, total)

    def whole(group, carry):
        per_group(group * 16, 16)
        return carry

    eights = lax.shift_right_logical(count + 7, 3)
    wholes = lax.shift_right_logical(eights, 1)
    lax.fori_loop(0, wholes, whole, 0)

    def rest(_, carry):
        per_group(wholes * 16, 8)
        return carry

    lax.fori_loop(0, lax.bitwise_and(eights, 1), rest, 0)


def row_sums(sums, local_cells):
    lane = lax.broadcasted_iota(jnp.int32, (LANES, LANES), 1)
    held = jnp.zeros((LANES, LANES), jnp.float32)
    for cell in range(local_cells):
        held = jnp.where(lane == cell, jnp.sum(sums[cell], axis=1, keepdims=True), held)
    return jnp.transpose(held)[:local_cells]


def prepare_kernel(counts_ref, particles_ref, lists_ref, sent_ref, padded_ref, own_ref):
    local_cells, columns = lists_ref.shape
    lane = lax.broadcasted_iota(jnp.int32, (1, LANES), 1)
    padded_ref[...] = jnp.full(padded_ref.shape, -1, jnp.int32)
    padded_ref[:, 0:columns] = lists_ref[...]
    for cell in range(local_cells):
        count = counts_ref[cell]
        row = slice(cell, cell + 1)
        for c, d in enumerate((0, 1, 2, None, 3, 4, 5)):
            if d is not None:
                sent_ref[cell, c : c + 1, :] = particles_ref[d, row, :]
        sent_ref[cell, 3:4, :] = jnp.where(lane < count, particles_ref[7, row, :], 0.0)
        sent_ref[cell, 7:8, :] = ((padded_ref[row, :] + 1) * 256 + count).astype(jnp.float32)
    smooth = particles_ref[6]
    steep = slope_norm ** (1.0 / 3.0) * jnp.exp((-5.0 / 3.0) * jnp.log(smooth))
    rows = [particles_ref[d] for d in range(6)] + [2.0 / smooth, smooth * 0.05, steep, steep * (0.5 / smooth)]
    for cell in range(local_cells):
        for c, row in enumerate(rows):
            own_ref[cell, c : c + 1, :] = row[cell : cell + 1]


def spread_kernel(rows_ref, after_ref, spread_ref):
    def per_pair(pair, carry):
        cells = (2 * pair, 2 * pair + 1)
        held = [jnp.transpose(rows_ref[cell]) for cell in cells]
        for c in range(spread_ref.shape[1]):
            for cell, columns in zip(cells, held):
                spread_ref[cell, c] = jnp.broadcast_to(columns[:, c : c + 1], (LANES, LANES))
        return carry

    lax.fori_loop(0, spread_ref.shape[0] // 2, per_pair, 0)


def partner_codes(place_ref, padded_ref, table_ref, code_ref, listed_ref, found_ref, columns, chips):
    local_cells = padded_ref.shape[0]
    reach = reach_of(local_cells)
    lane = lax.broadcasted_iota(jnp.int32, (1, LANES), 1)
    inner = lax.broadcasted_iota(jnp.int32, (8, LANES), 0)
    starts = window_starts(place_ref[0], place_ref[1], local_cells, reach)
    groups = []
    for first in range(0, table_ref.shape[0], 8):
        start, where = starts[first // local_cells]
        span = slice(first, first + 8)
        lists = table_ref[span, 7, :].astype(jnp.int32)
        real = (where >= 0) & (where < chips)
        count = lax.bitwise_and(lists, 255)
        code_ref[span, :] = jnp.where(real, (inner + first) * 256 + count, 0).astype(jnp.float32)
        listed_ref[span, :] = (lax.shift_right_logical(lists, 8) - 1).astype(jnp.float32)
        groups.append((span, start + first % local_cells))
    own_start = starts[0][0]

    def per_cell(cell, carry):
        own = own_start + cell
        row = padded_ref[pl.ds(cell, 1), :]
        wanted = jnp.where(lane == columns, own, jnp.where(row >= 0, row, -(1 << 20)))
        ahead = jnp.zeros((8, LANES), jnp.float32)
        behind = jnp.zeros((8, LANES), jnp.float32)
        for span, start in groups:
            code = code_ref[span, :]
            ahead = jnp.maximum(ahead, jnp.where(inner == wanted - start, code, 0.0))
            behind = jnp.maximum(behind, jnp.where(listed_ref[span, :] == own.astype(jnp.float32), code, 0.0))
        ahead = jnp.max(ahead, axis=0, keepdims=True)
        behind = pltpu.roll(jnp.max(behind, axis=0, keepdims=True), columns + 1, 1)
        found_ref[pl.ds(cell, 1), :] = jnp.where(lane <= columns, ahead, behind).astype(jnp.int32)
        return carry

    lax.fori_loop(0, local_cells, per_cell, 0)


def density_kernel(
    place_ref, counts_ref, padded_ref, table_ref, particles_ref, own_ref, spread_ref,
    out_ref, state_ref, pack_ref, codes_ref, sums_ref, code_ref, listed_ref, found_ref, *, columns, chips,
):
    local_cells = particles_ref.shape[1]
    partner_codes(place_ref, padded_ref, table_ref, code_ref, listed_ref, found_ref, columns, chips)
    pltpu.sync_copy(found_ref, codes_ref)

    def per_cell(cell, carry):
        tile_count = pack_sources(cell, codes_ref, columns, [table_ref], [pack_ref.at[cell]], 2)

        def body(span):
            xa, ya, za, ia = (spread_ref[cell, c, span, :] for c in (0, 1, 2, 6))

            def step(first, tiles, total):
                for u in range(tiles):
                    at = first + u
                    dx = xa - pack_ref[cell, at, 0:1, :]
                    dy = ya - pack_ref[cell, at, 1:2, :]
                    dz = za - pack_ref[cell, at, 2:3, :]
                    squared = dx * dx + dy * dy + dz * dz
                    scaled = squared * lax.rsqrt(jnp.maximum(squared, TINY)) * ia
                    remain = jnp.maximum(4.0 - scaled, 0.0)
                    remain = remain * remain
                    total = total + remain * remain * ((1.0 + scaled) * pack_ref[cell, at, 3:4, :])
                return total

            return step

        def finish(span, total):
            sums_ref[cell, span, :] = total

        each_group(counts_ref[cell], tile_count, body, finish, lambda rows: jnp.zeros((rows, LANES), jnp.float32))
        return carry

    lax.fori_loop(0, local_cells, per_cell, 0)
    raw = row_sums(sums_ref, local_cells)
    masses = jnp.concatenate([table_ref[cell, 3:4, :] for cell in range(local_cells)], axis=0)
    smooth, entropy = particles_ref[6], particles_ref[8]
    held = masses > 0.0
    smooth = jnp.where(held, smooth, 1.0)
    density = jnp.where(held, raw * (kernel_norm / 256.0) / (smooth * smooth * smooth), 0.0)
    out_ref[...] = density
    bounded = jnp.where(held, density, 1.0)
    log_density = jnp.log(bounded)
    pressure_term = entropy * jnp.exp((gamma_index - 2.0) * log_density)
    sound = jnp.sqrt(gamma_index * entropy * jnp.exp((gamma_index - 1.0) * log_density))
    rows = (bounded * 0.005, pressure_term, sound * 0.025)
    for cell in range(local_cells):
        for c, row in enumerate(rows):
            state_ref[cell, c : c + 1, :] = row[cell : cell + 1]
        state_ref[cell, 3:6, :] = own_ref[cell, 7:10, :]
        state_ref[cell, 6:8, :] = jnp.zeros((2, LANES), jnp.float32)


def force_kernel(
    counts_ref, codes_ref, table_ref, state_ref, pack_ref, spread_ref, state_spread_ref,
    out_ref, state_pack_ref, sums_ref, *, columns,
):
    local_cells = out_ref.shape[1]

    def per_cell(cell, carry):
        tile_count = pack_sources(cell, codes_ref, columns, [state_ref], [state_pack_ref], 2)

        def body(span):
            def step(first, tiles, total):
                for u in range(tiles):
                    at = first + u
                    xa, ya, za, ua, va, wa = (spread_ref[cell, c, span, :] for c in range(6))
                    ga, sa, ja = (spread_ref[cell, c, span, :] for c in range(7, 10))
                    ra, fa, ca = (state_spread_ref[cell, c, span, :] for c in range(3))
                    xb, yb, zb, mb, ub, vb, wb = (pack_ref[cell, at, c : c + 1, :] for c in range(7))
                    rb, fb, cb, gb, sb, jb = (state_pack_ref[at, c : c + 1, :] for c in range(6))
                    dx, dy, dz = xa - xb, ya - yb, za - zb
                    squared = dx * dx + dy * dy + dz * dz
                    apart = squared * lax.rsqrt(jnp.maximum(squared, TINY))
                    closing = (ua - ub) * dx + (va - vb) * dy + (wa - wb) * dz
                    slope_a = jnp.maximum(sa - apart * ja, 0.0)
                    slope_a = slope_a * slope_a * slope_a
                    slope_b = jnp.maximum(sb - apart * jb, 0.0)
                    slope_b = slope_b * slope_b * slope_b
                    width = ga + gb
                    approach = jnp.minimum(width * closing, 0.0) / (squared + width * width)
                    viscous = approach * (approach - (ca + cb)) / (ra + rb)
                    coupling = ((fa + viscous) * slope_a + (fb + viscous) * slope_b) * mb
                    total = (total[0] + coupling * dx, total[1] + coupling * dy, total[2] + coupling * dz)
                return total

            return step

        def finish(span, total):
            for d in range(3):
                sums_ref[d, cell, span, :] = total[d]

        each_group(
            counts_ref[cell], tile_count, body, finish, lambda rows: (jnp.zeros((rows, LANES), jnp.float32),) * 3
        )
        return carry

    lax.fori_loop(0, local_cells, per_cell, 0)
    held = jnp.concatenate([table_ref[cell, 3:4, :] for cell in range(local_cells)], axis=0) > 0.0
    for d in range(3):
        out_ref[d] = jnp.where(held, row_sums(sums_ref.at[d], local_cells), 0.0)


def on_chip(array):
    return pltpu.with_memory_space_constraint(array, pltpu.VMEM)


def per_device(particles, counts, pair_lists):
    local_cells, _, slots = particles.shape
    columns = pair_lists.shape[1]
    assert slots == LANES and local_cells % 8 == 0
    scalars = pl.BlockSpec(memory_space=pltpu.SMEM)
    whole = pl.BlockSpec(memory_space=pltpu.VMEM)
    plain = lambda *shape: jax.ShapeDtypeStruct(shape, jnp.float32)
    floats = lambda *shape: pltpu.VMEM(shape, jnp.float32)
    chips = lax.axis_size("curve")
    place = jnp.stack([lax.axis_index("curve"), lax.axis_index("group")]).astype(jnp.int32)
    particles = jnp.transpose(particles, (1, 0, 2))
    sent, padded, own = pl.pallas_call(
        prepare_kernel,
        out_shape=(plain(local_cells, 8, slots), pltpu.VMEM((local_cells, LANES), jnp.int32), floats(local_cells, 16, slots)),
        in_specs=[scalars, whole, whole],
        out_specs=(whole, whole, whole),
        name="prepare",
        compiler_params=pltpu.CompilerParams(vmem_limit_bytes=ROOM),
    )(counts, particles, pair_lists)

    def spread(rows, channels, after):
        return pl.pallas_call(
            spread_kernel,
            out_shape=floats(local_cells, channels, LANES, LANES),
            in_specs=[whole, pl.BlockSpec(memory_space=pl.ANY)],
            out_specs=whole,
            name="spread",
        compiler_params=pltpu.CompilerParams(vmem_limit_bytes=ROOM),
        )(rows, after)

    window, own_spread = surround(sent, lambda after: spread(own, 10, after))
    table = on_chip(window)
    most_tiles = 2 * columns + 5
    rows = table.shape[0]
    density, state, packed, codes = pl.pallas_call(
        lambda *refs: density_kernel(*refs, columns=columns, chips=chips),
        out_shape=(
            plain(local_cells, slots),
            plain(local_cells, 8, slots),
            floats(local_cells, most_tiles, 8, LANES),
            jax.ShapeDtypeStruct((local_cells, LANES), jnp.int32),
        ),
        in_specs=[scalars, scalars, whole, whole, whole, whole, whole],
        out_specs=(whole, whole, whole, scalars),
        scratch_shapes=[
            floats(local_cells, LANES, LANES),
            floats(rows, LANES),
            floats(rows, LANES),
            pltpu.VMEM((local_cells, LANES), jnp.int32),
        ],
        name="density_sweep",
        compiler_params=pltpu.CompilerParams(vmem_limit_bytes=ROOM),
    )(place, counts, padded, table, particles, own, own_spread)
    states, state_spread = surround(state, lambda after: spread(state, 3, after))
    acceleration = pl.pallas_call(
        lambda *refs: force_kernel(*refs, columns=columns),
        out_shape=plain(3, local_cells, slots),
        in_specs=[scalars, scalars, whole, whole, whole, whole, whole],
        out_specs=whole,
        scratch_shapes=[floats(most_tiles, 8, LANES), floats(3, local_cells, LANES, LANES)],
        name="force_sweep",
        compiler_params=pltpu.CompilerParams(vmem_limit_bytes=ROOM),
    )(counts, codes, table, on_chip(states), packed, own_spread, state_spread)
    return density, jnp.transpose(acceleration, (1, 0, 2))


def solution(mesh):
    in_specs = (P(AXES, None, None), P(AXES), P(AXES, None))
    out_specs = (P(AXES, None), P(AXES, None, None))
    return jax.shard_map(per_device, mesh=mesh, in_specs=in_specs, out_specs=out_specs, check_vma=False)
```

```python
import jax
import jax.numpy as jnp
from jax import lax
from jax.experimental import pallas as pl
from jax.experimental.pallas import tpu as pltpu
from jax.sharding import PartitionSpec as P


FARTHEST = 127

gamma_index = 5.0 / 3.0
kernel_norm = 21.0 / (2.0 * 3.141592653589793)
slope_norm = 105.0 / (2.0 * 3.141592653589793)

LANES = 128
ROOM = 12 << 20
TINY = 1.2e-38
AXES = ("curve", "group")


def swap_cores(block):
    return lax.ppermute(block, "group", [(0, 1), (1, 0)])


def reach_of(local_cells):
    return -(-FARTHEST // (2 * local_cells))


def route_of(chips, k):
    route = []
    for chip in range(chips):
        route.append((2 * (chip + k) if chip + k < chips else 2 * chip + 1, 2 * chip))
        route.append((2 * (chip - k) + 1 if chip - k >= 0 else 2 * chip, 2 * chip + 1))
    return route


def surround(block, beside):
    chips = lax.axis_size("curve")
    chip_block = jnp.concatenate([block, swap_cores(block)], axis=0)
    reach = reach_of(block.shape[0])
    fetched = []
    for k in range(1, reach + 1):
        fetched.append(lax.ppermute(chip_block, AXES, route_of(chips, k)))
    made = beside(chip_block)
    fetched = jnp.concatenate(fetched, axis=0)
    return jnp.concatenate([chip_block, fetched, swap_cores(fetched)], axis=0), made


def window_starts(chip, core, local_cells, reach):
    side = 1 - 2 * core
    runs = [(chip, core), (chip, 1 - core)]
    for k in range(1, reach + 1):
        runs += [(chip + side * k, core), (chip + side * k, 1 - core)]
    for k in range(1, reach + 1):
        runs += [(chip - side * k, 1 - core), (chip - side * k, core)]
    return [((2 * where + half) * local_cells, where) for where, half in runs]


def pack_sources(cell, local_cells, index_ref, entries, table, lift, pack, pad_tiles):
    lane = lax.broadcasted_iota(jnp.int32, (1, LANES), 1)
    held = jnp.zeros(pack.shape[1:], jnp.float32)
    tile = index_ref[local_cells + cell, 0]
    for entry in range(entries):
        turn = index_ref[2 * local_cells + cell, entry]
        following = index_ref[local_cells + cell, entry + 1]
        rolled = pltpu.roll(lift(table[index_ref[cell, entry]]), turn, 1)
        merged = jnp.where(lane >= turn, rolled, held)
        pack[tile] = merged
        held = jnp.where(following > tile, rolled, merged)
        tile = following
    turn = index_ref[2 * local_cells + cell, entries]
    pack[tile] = jnp.where(lane < turn, held, 0.0)
    for extra in range(1, pad_tiles):
        pack[tile + extra] = jnp.zeros(pack.shape[1:], jnp.float32)
    return jnp.where(turn > 0, tile + 1, tile)


def count_of(cell, local_cells, index_ref, entry):
    tiles = index_ref[local_cells + cell, entry + 1] - index_ref[local_cells + cell, entry]
    return 128 * tiles + index_ref[2 * local_cells + cell, entry + 1] - index_ref[2 * local_cells + cell, entry]


def each_group(count, tile_count, body, finish, zeros):
    fours = lax.shift_right_logical(tile_count + 1, 2)
    twos = jnp.where(tile_count > 4 * fours, 1, 0)

    def per_group(start, rows):
        span = pl.ds(pl.multiple_of(start, 8), rows)
        step = body(span)
        total = zeros(rows)
        total = lax.fori_loop(0, fours, lambda k, t: step(4 * k, 4, t), total)
        total = lax.fori_loop(0, twos, lambda k, t: step(4 * fours, 2, t), total)
        finish(span, total)

    def whole(group, carry):
        per_group(group * 16, 16)
        return carry

    eights = lax.shift_right_logical(count + 7, 3)
    wholes = lax.shift_right_logical(eights, 1)
    lax.fori_loop(0, wholes, whole, 0)

    def rest(_, carry):
        per_group(wholes * 16, 8)
        return carry

    lax.fori_loop(0, lax.bitwise_and(eights, 1), rest, 0)


def row_sums(sums, local_cells):
    lane = lax.broadcasted_iota(jnp.int32, (LANES, LANES), 1)
    held = jnp.zeros((LANES, LANES), jnp.float32)
    for cell in range(local_cells):
        held = jnp.where(lane == cell, jnp.sum(sums[cell], axis=1, keepdims=True), held)
    return jnp.transpose(held)[:local_cells]


def prepare_kernel(counts_ref, particles_ref, lists_ref, sent_ref, padded_ref, own_ref):
    local_cells, columns = lists_ref.shape
    lane = lax.broadcasted_iota(jnp.int32, (1, LANES), 1)
    padded_ref[...] = jnp.full(padded_ref.shape, -1, jnp.int32)
    padded_ref[:, 0:columns] = lists_ref[...]
    for cell in range(local_cells):
        count = counts_ref[cell]
        row = slice(cell, cell + 1)
        for c, d in enumerate((0, 1, 2, None, 3, 4, 5)):
            if d is not None:
                sent_ref[cell, c : c + 1, :] = particles_ref[d, row, :]
        sent_ref[cell, 3:4, :] = jnp.where(lane < count, particles_ref[7, row, :], 0.0)
        sent_ref[cell, 7:8, :] = ((padded_ref[row, :] + 1) * 256 + count).astype(jnp.float32)
    smooth = particles_ref[6]
    steep = slope_norm ** (1.0 / 3.0) * jnp.exp((-5.0 / 3.0) * jnp.log(smooth))
    rows = [particles_ref[d] for d in range(6)]
    rows += [2.0 / smooth, smooth * 0.05, steep, steep * (0.5 / smooth), smooth, particles_ref[8]]
    for cell in range(local_cells):
        for c, row in enumerate(rows):
            own_ref[cell, c : c + 1, :] = row[cell : cell + 1]


def spread_kernel(rows_ref, after_ref, spread_ref):
    def per_pair(pair, carry):
        cells = (2 * pair, 2 * pair + 1)
        held = [jnp.transpose(rows_ref[cell]) for cell in cells]
        for c in range(spread_ref.shape[1]):
            for cell, columns in zip(cells, held):
                spread_ref[cell, c] = jnp.broadcast_to(columns[:, c : c + 1], (LANES, LANES))
        return carry

    lax.fori_loop(0, spread_ref.shape[0] // 2, per_pair, 0)


def find_partners(padded_ref, table_ref, code_ref, listed_ref, found_ref, columns):
    chips = lax.axis_size("curve")
    local_cells = padded_ref.shape[0]
    reach = reach_of(local_cells)
    lane = lax.broadcasted_iota(jnp.int32, (1, LANES), 1)
    inner = lax.broadcasted_iota(jnp.int32, (8, LANES), 0)
    starts = window_starts(lax.axis_index("curve"), lax.axis_index("group"), local_cells, reach)
    groups = []
    for first in range(0, table_ref.shape[0], 8):
        start, where = starts[first // local_cells]
        span = slice(first, first + 8)
        lists = table_ref[span, 7, :].astype(jnp.int32)
        real = (where >= 0) & (where < chips)
        count = lax.bitwise_and(lists, 255)
        code_ref[span, :] = jnp.where(real, (inner + first) * 256 + count, 0).astype(jnp.float32)
        listed_ref[span, :] = (lax.shift_right_logical(lists, 8) - 1).astype(jnp.float32)
        groups.append((span, start + first % local_cells))
    own_start = starts[0][0]

    def per_cell(cell, carry):
        own = own_start + cell
        row = padded_ref[pl.ds(cell, 1), :]
        wanted = jnp.where(lane == columns, own, jnp.where(row >= 0, row, -(1 << 20)))
        ahead = jnp.zeros((8, LANES), jnp.float32)
        behind = jnp.zeros((8, LANES), jnp.float32)
        for span, start in groups:
            code = code_ref[span, :]
            ahead = jnp.maximum(ahead, jnp.where(inner == wanted - start, code, 0.0))
            behind = jnp.maximum(behind, jnp.where(listed_ref[span, :] == own.astype(jnp.float32), code, 0.0))
        ahead = jnp.max(ahead, axis=0, keepdims=True)
        behind = pltpu.roll(jnp.max(behind, axis=0, keepdims=True), columns + 1, 1)
        found_ref[pl.ds(cell, 1), :] = jnp.where(lane <= columns, ahead, behind).astype(jnp.int32)
        return carry

    lax.fori_loop(0, local_cells, per_cell, 0)
    code = found_ref[0:local_cells, :]
    count = lax.bitwise_and(code, 255)
    place, shift = count, 1
    while shift < 2 * columns + 1:
        place = place + jnp.where(lane >= shift, pltpu.roll(place, shift, 1), 0)
        shift *= 2
    place = place - count
    found_ref[0:local_cells, :] = lax.shift_right_logical(code, 8)
    found_ref[local_cells : 2 * local_cells, :] = lax.shift_right_logical(place, 7)
    found_ref[2 * local_cells : 3 * local_cells, :] = lax.bitwise_and(place, 127)


def density_kernel(
    padded_ref, table_ref, own_ref, spread_ref,
    out_ref, sent_ref, state_ref, pack_ref, index_ref, sums_ref, code_ref, listed_ref, found_ref, *, columns,
):
    local_cells = out_ref.shape[0]
    entries = 2 * columns + 1
    find_partners(padded_ref, table_ref, code_ref, listed_ref, found_ref, columns)
    pltpu.sync_copy(found_ref, index_ref)

    def per_cell(cell, carry):
        tile_count = pack_sources(
            cell, local_cells, index_ref, entries, table_ref, lambda held: held, pack_ref.at[cell], 2
        )
        count = count_of(cell, local_cells, index_ref, columns)

        def body(span):
            xa, ya, za, ia = (spread_ref[cell, c, span, :] for c in (0, 1, 2, 6))

            def step(first, tiles, total):
                for u in range(tiles):
                    at = first + u
                    dx = xa - pack_ref[cell, at, 0:1, :]
                    dy = ya - pack_ref[cell, at, 1:2, :]
                    dz = za - pack_ref[cell, at, 2:3, :]
                    squared = dx * dx + dy * dy + dz * dz
                    scaled = squared * lax.rsqrt(jnp.maximum(squared, TINY)) * ia
                    remain = jnp.maximum(4.0 - scaled, 0.0)
                    remain = remain * remain
                    total = total + remain * remain * ((1.0 + scaled) * pack_ref[cell, at, 3:4, :])
                return total

            return step

        def finish(span, total):
            sums_ref[cell, span, :] = total

        each_group(count, tile_count, body, finish, lambda rows: jnp.zeros((rows, LANES), jnp.float32))
        return carry

    lax.fori_loop(0, local_cells, per_cell, 0)
    raw = row_sums(sums_ref, local_cells)
    masses = jnp.concatenate([table_ref[cell, 3:4, :] for cell in range(local_cells)], axis=0)
    smooth = jnp.concatenate([own_ref[cell, 10:11, :] for cell in range(local_cells)], axis=0)
    entropy = jnp.concatenate([own_ref[cell, 11:12, :] for cell in range(local_cells)], axis=0)
    held = masses > 0.0
    smooth = jnp.where(held, smooth, 1.0)
    density = jnp.where(held, raw * (kernel_norm / 256.0) / (smooth * smooth * smooth), 0.0)
    out_ref[...] = density
    bounded = jnp.where(held, density, 1.0)
    log_density = jnp.log(bounded)
    pressure_term = entropy * jnp.exp((gamma_index - 2.0) * log_density)
    sound = jnp.sqrt(gamma_index * entropy * jnp.exp((gamma_index - 1.0) * log_density))
    rows = (bounded * 0.005, pressure_term, sound * 0.025)
    for cell in range(local_cells):
        for c, row in enumerate(rows):
            state_ref[cell, c : c + 1, :] = row[cell : cell + 1]
        state_ref[cell, 3:8, :] = jnp.zeros((5, LANES), jnp.float32)
        for c in range(2):
            sent_ref[cell, c : c + 1, :] = rows[c][cell : cell + 1]
        sent_ref[cell, 2:3, :] = own_ref[cell, 8:9, :]
        sent_ref[cell, 3:4, :] = own_ref[cell, 7:8, :]


def with_sound(held):
    squared = (0.025 * 0.025 * 200.0 * gamma_index) * (held[0:1] * held[1:2])
    sound = squared * lax.rsqrt(jnp.maximum(squared, TINY))
    return jnp.concatenate([held, sound, 0.025 * held[2:3] / held[3:4]], axis=0)


def force_kernel(
    index_ref, table_ref, state_ref, pack_ref, spread_ref, state_spread_ref,
    out_ref, state_pack_ref, sums_ref, *, columns,
):
    local_cells = out_ref.shape[1]
    entries = 2 * columns + 1

    def per_cell(cell, carry):
        tile_count = pack_sources(
            cell, local_cells, index_ref, entries, state_ref, with_sound, state_pack_ref, 2
        )
        count = count_of(cell, local_cells, index_ref, columns)

        def body(span):
            def step(first, tiles, total):
                for u in range(tiles):
                    at = first + u
                    xa, ya, za, ua, va, wa = (spread_ref[cell, c, span, :] for c in range(6))
                    ga, sa, ja = (spread_ref[cell, c, span, :] for c in range(7, 10))
                    ra, fa, ca = (state_spread_ref[cell, c, span, :] for c in range(3))
                    xb, yb, zb, mb, ub, vb, wb = (pack_ref[cell, at, c : c + 1, :] for c in range(7))
                    rb, fb, sb, gb, cb, jb = (state_pack_ref[at, c : c + 1, :] for c in range(6))
                    dx, dy, dz = xa - xb, ya - yb, za - zb
                    squared = dx * dx + dy * dy + dz * dz
                    apart = squared * lax.rsqrt(jnp.maximum(squared, TINY))
                    closing = (ua - ub) * dx + (va - vb) * dy + (wa - wb) * dz
                    slope_a = jnp.maximum(sa - apart * ja, 0.0)
                    slope_a = slope_a * slope_a * slope_a
                    slope_b = jnp.maximum(sb - apart * jb, 0.0)
                    slope_b = slope_b * slope_b * slope_b
                    width = ga + gb
                    approach = jnp.minimum(width * closing, 0.0) / (squared + width * width)
                    viscous = approach * (approach - (ca + cb)) / (ra + rb)
                    coupling = ((fa + viscous) * slope_a + (fb + viscous) * slope_b) * mb
                    total = (total[0] + coupling * dx, total[1] + coupling * dy, total[2] + coupling * dz)
                return total

            return step

        def finish(span, total):
            for d in range(3):
                sums_ref[d, cell, span, :] = total[d]

        each_group(
            count, tile_count, body, finish, lambda rows: (jnp.zeros((rows, LANES), jnp.float32),) * 3
        )
        return carry

    lax.fori_loop(0, local_cells, per_cell, 0)
    held = jnp.concatenate([table_ref[cell, 3:4, :] for cell in range(local_cells)], axis=0) > 0.0
    for d in range(3):
        out_ref[d] = jnp.where(held, row_sums(sums_ref.at[d], local_cells), 0.0)


def on_chip(array):
    return pltpu.with_memory_space_constraint(array, pltpu.VMEM)


def off_chip(array):
    return pltpu.with_memory_space_constraint(array, pltpu.HBM)


def per_device(particles, counts, pair_lists):
    local_cells, _, slots = particles.shape
    columns = pair_lists.shape[1]
    assert slots == LANES and local_cells % 8 == 0
    scalars = pl.BlockSpec(memory_space=pltpu.SMEM)
    whole = pl.BlockSpec(memory_space=pltpu.VMEM)
    plain = lambda *shape: jax.ShapeDtypeStruct(shape, jnp.float32)
    floats = lambda *shape: pltpu.VMEM(shape, jnp.float32)
    particles = jnp.transpose(particles, (1, 0, 2))
    sent, padded, own = pl.pallas_call(
        prepare_kernel,
        out_shape=(plain(local_cells, 8, slots), pltpu.VMEM((local_cells, LANES), jnp.int32), floats(local_cells, 16, slots)),
        in_specs=[scalars, whole, whole],
        out_specs=(whole, whole, whole),
        name="prepare",
        compiler_params=pltpu.CompilerParams(vmem_limit_bytes=ROOM),
    )(counts, off_chip(particles), off_chip(pair_lists))

    def spread(rows, channels, after):
        return pl.pallas_call(
            spread_kernel,
            out_shape=floats(local_cells, channels, LANES, LANES),
            in_specs=[whole, pl.BlockSpec(memory_space=pl.ANY)],
            out_specs=whole,
            name="spread",
        compiler_params=pltpu.CompilerParams(vmem_limit_bytes=ROOM),
        )(rows, after)

    window, own_spread = surround(sent, lambda after: spread(own, 10, after))
    table = on_chip(window)
    most_tiles = 2 * columns + 5
    rows = table.shape[0]
    density, thermal, state, packed, index = pl.pallas_call(
        lambda *refs: density_kernel(*refs, columns=columns),
        out_shape=(
            plain(local_cells, slots),
            plain(local_cells, 4, slots),
            floats(local_cells, 8, slots),
            floats(local_cells, most_tiles, 8, LANES),
            jax.ShapeDtypeStruct((3 * local_cells, LANES), jnp.int32),
        ),
        in_specs=[whole, whole, whole, whole],
        out_specs=(whole, whole, whole, whole, scalars),
        scratch_shapes=[
            floats(local_cells, LANES, LANES),
            floats(rows, LANES),
            floats(rows, LANES),
            pltpu.VMEM((3 * local_cells, LANES), jnp.int32),
        ],
        name="density_sweep",
        compiler_params=pltpu.CompilerParams(vmem_limit_bytes=ROOM),
    )(padded, table, own, own_spread)
    states, state_spread = surround(thermal, lambda after: spread(state, 3, after))
    acceleration = pl.pallas_call(
        lambda *refs: force_kernel(*refs, columns=columns),
        out_shape=plain(3, local_cells, slots),
        in_specs=[scalars, whole, whole, whole, whole, whole],
        out_specs=whole,
        scratch_shapes=[floats(most_tiles, 6, LANES), floats(3, local_cells, LANES, LANES)],
        name="force_sweep",
        compiler_params=pltpu.CompilerParams(vmem_limit_bytes=ROOM),
    )(index, table, on_chip(states), packed, own_spread, state_spread)
    return density, jnp.transpose(acceleration, (1, 0, 2))


def solution(mesh):
    in_specs = (P(AXES, None, None), P(AXES), P(AXES, None))
    out_specs = (P(AXES, None), P(AXES, None, None))
    return jax.shard_map(per_device, mesh=mesh, in_specs=in_specs, out_specs=out_specs, check_vma=False)
```

```python
import jax
import jax.numpy as jnp
from jax import lax
from jax.experimental import pallas as pl
from jax.experimental.pallas import tpu as pltpu
from jax.sharding import PartitionSpec as P


FARTHEST = 127

gamma_index = 5.0 / 3.0
kernel_norm = 21.0 / (2.0 * 3.141592653589793)
slope_norm = 105.0 / (2.0 * 3.141592653589793)

LANES = 128
ROOM = 12 << 20
TINY = 1.2e-38
AXES = ("curve", "group")


def swap_cores(block):
    return lax.ppermute(block, "group", [(0, 1), (1, 0)])


def reach_of(local_cells):
    return -(-FARTHEST // (2 * local_cells))


def route_of(chips, k):
    route = []
    for chip in range(chips):
        route.append((2 * (chip + k) if chip + k < chips else 2 * chip + 1, 2 * chip))
        route.append((2 * (chip - k) + 1 if chip - k >= 0 else 2 * chip, 2 * chip + 1))
    return route


def surround(block, beside):
    chips = lax.axis_size("curve")
    chip_block = jnp.concatenate([block, swap_cores(block)], axis=0)
    reach = reach_of(block.shape[0])
    fetched = []
    for k in range(1, reach + 1):
        fetched.append(lax.ppermute(chip_block, AXES, route_of(chips, k)))
    made = beside(chip_block)
    fetched = jnp.concatenate(fetched, axis=0)
    return jnp.concatenate([chip_block, fetched, swap_cores(fetched)], axis=0), made


def window_starts(chip, core, local_cells, reach):
    side = 1 - 2 * core
    runs = [(chip, core), (chip, 1 - core)]
    for k in range(1, reach + 1):
        runs += [(chip + side * k, core), (chip + side * k, 1 - core)]
    for k in range(1, reach + 1):
        runs += [(chip - side * k, 1 - core), (chip - side * k, core)]
    return [((2 * where + half) * local_cells, where) for where, half in runs]


def pack_sources(cell, local_cells, index_ref, entries, table, lift, pack, pad_tiles):
    lane = lax.broadcasted_iota(jnp.int32, (1, LANES), 1)
    held = jnp.zeros(pack.shape[1:], jnp.float32)
    tile = index_ref[local_cells + cell, 0]
    for entry in range(entries):
        turn = index_ref[2 * local_cells + cell, entry]
        following = index_ref[local_cells + cell, entry + 1]
        rolled = pltpu.roll(lift(table[index_ref[cell, entry]]), turn, 1)
        merged = jnp.where(lane >= turn, rolled, held)
        pack[tile] = merged
        held = jnp.where(following > tile, rolled, merged)
        tile = following
    turn = index_ref[2 * local_cells + cell, entries]
    pack[tile] = jnp.where(lane < turn, held, 0.0)
    for extra in range(1, pad_tiles):
        pack[tile + extra] = jnp.zeros(pack.shape[1:], jnp.float32)
    return jnp.where(turn > 0, tile + 1, tile)


def count_of(cell, local_cells, index_ref, entry):
    tiles = index_ref[local_cells + cell, entry + 1] - index_ref[local_cells + cell, entry]
    return 128 * tiles + index_ref[2 * local_cells + cell, entry + 1] - index_ref[2 * local_cells + cell, entry]


def each_group(count, tile_count, body, finish, zeros):
    fours = lax.shift_right_logical(tile_count + 1, 2)
    twos = jnp.where(tile_count > 4 * fours, 1, 0)

    def per_group(start, rows):
        span = pl.ds(pl.multiple_of(start, 8), rows)
        step = body(span)
        total = zeros(rows)
        total = lax.fori_loop(0, fours, lambda k, t: step(4 * k, 4, t), total)
        total = lax.fori_loop(0, twos, lambda k, t: step(4 * fours, 2, t), total)
        finish(span, total)

    start = jnp.int32(0)
    eights = lax.shift_right_logical(count + 7, 3)
    for rows, groups in (
        (32, lax.shift_right_logical(eights, 2)),
        (16, lax.bitwise_and(lax.shift_right_logical(eights, 1), 1)),
        (8, lax.bitwise_and(eights, 1)),
    ):

        def several(group, carry, start=start, rows=rows):
            per_group(start + group * rows, rows)
            return carry

        lax.fori_loop(0, groups, several, 0)
        start = start + groups * rows


def row_sums(sums, local_cells):
    lane = lax.broadcasted_iota(jnp.int32, (LANES, LANES), 1)
    held = jnp.zeros((LANES, LANES), jnp.float32)
    for cell in range(local_cells):
        held = jnp.where(lane == cell, jnp.sum(sums[cell], axis=1, keepdims=True), held)
    return jnp.transpose(held)[:local_cells]


def prepare_kernel(counts_ref, particles_ref, lists_ref, sent_ref, padded_ref, own_ref):
    local_cells, columns = lists_ref.shape
    lane = lax.broadcasted_iota(jnp.int32, (1, LANES), 1)
    padded_ref[...] = jnp.full(padded_ref.shape, -1, jnp.int32)
    padded_ref[:, 0:columns] = lists_ref[...]
    for cell in range(local_cells):
        count = counts_ref[cell]
        row = slice(cell, cell + 1)
        for c, d in enumerate((0, 1, 2, None, 3, 4, 5)):
            if d is not None:
                sent_ref[cell, c : c + 1, :] = particles_ref[d, row, :]
        sent_ref[cell, 3:4, :] = jnp.where(lane < count, particles_ref[7, row, :], 0.0)
        sent_ref[cell, 7:8, :] = ((padded_ref[row, :] + 1) * 256 + count).astype(jnp.float32)
    smooth = particles_ref[6]
    steep = slope_norm ** (1.0 / 3.0) * jnp.exp((-5.0 / 3.0) * jnp.log(smooth))
    rows = [particles_ref[d] for d in range(6)]
    rows += [2.0 / smooth, smooth * 0.05, steep, steep * (0.5 / smooth), smooth, particles_ref[8]]
    for cell in range(local_cells):
        for c, row in enumerate(rows):
            own_ref[cell, c : c + 1, :] = row[cell : cell + 1]


def spread_kernel(rows_ref, after_ref, spread_ref):
    def per_pair(pair, carry):
        cells = (2 * pair, 2 * pair + 1)
        held = [jnp.transpose(rows_ref[cell]) for cell in cells]
        for c in range(spread_ref.shape[1]):
            for cell, columns in zip(cells, held):
                spread_ref[cell, c] = jnp.broadcast_to(columns[:, c : c + 1], (LANES, LANES))
        return carry

    lax.fori_loop(0, spread_ref.shape[0] // 2, per_pair, 0)


def find_partners(padded_ref, table_ref, code_ref, listed_ref, found_ref, columns):
    chips = lax.axis_size("curve")
    local_cells = padded_ref.shape[0]
    reach = reach_of(local_cells)
    lane = lax.broadcasted_iota(jnp.int32, (1, LANES), 1)
    inner = lax.broadcasted_iota(jnp.int32, (8, LANES), 0)
    starts = window_starts(lax.axis_index("curve"), lax.axis_index("group"), local_cells, reach)
    groups = []
    for first in range(0, table_ref.shape[0], 8):
        start, where = starts[first // local_cells]
        span = slice(first, first + 8)
        lists = table_ref[span, 7, :].astype(jnp.int32)
        real = (where >= 0) & (where < chips)
        count = lax.bitwise_and(lists, 255)
        code_ref[span, :] = jnp.where(real, (inner + first) * 256 + count, 0).astype(jnp.float32)
        listed_ref[span, :] = (lax.shift_right_logical(lists, 8) - 1).astype(jnp.float32)
        groups.append((span, start + first % local_cells))
    own_start = starts[0][0]

    def per_cell(cell, carry):
        own = own_start + cell
        row = padded_ref[pl.ds(cell, 1), :]
        wanted = jnp.where(lane == columns, own, jnp.where(row >= 0, row, -(1 << 20)))
        ahead = jnp.zeros((8, LANES), jnp.float32)
        behind = jnp.zeros((8, LANES), jnp.float32)
        for span, start in groups:
            code = code_ref[span, :]
            ahead = jnp.maximum(ahead, jnp.where(inner == wanted - start, code, 0.0))
            behind = jnp.maximum(behind, jnp.where(listed_ref[span, :] == own.astype(jnp.float32), code, 0.0))
        ahead = jnp.max(ahead, axis=0, keepdims=True)
        behind = pltpu.roll(jnp.max(behind, axis=0, keepdims=True), columns + 1, 1)
        found_ref[pl.ds(cell, 1), :] = jnp.where(lane <= columns, ahead, behind).astype(jnp.int32)
        return carry

    lax.fori_loop(0, local_cells, per_cell, 0)
    code = found_ref[0:local_cells, :]
    count = lax.bitwise_and(code, 255)
    place, shift = count, 1
    while shift < 2 * columns + 1:
        place = place + jnp.where(lane >= shift, pltpu.roll(place, shift, 1), 0)
        shift *= 2
    place = place - count
    found_ref[0:local_cells, :] = lax.shift_right_logical(code, 8)
    found_ref[local_cells : 2 * local_cells, :] = lax.shift_right_logical(place, 7)
    found_ref[2 * local_cells : 3 * local_cells, :] = lax.bitwise_and(place, 127)


def density_kernel(
    padded_ref, table_ref, own_ref, spread_ref,
    out_ref, sent_ref, state_ref, pack_ref, index_ref, sums_ref, code_ref, listed_ref, found_ref, *, columns,
):
    local_cells = out_ref.shape[0]
    entries = 2 * columns + 1
    find_partners(padded_ref, table_ref, code_ref, listed_ref, found_ref, columns)
    pltpu.sync_copy(found_ref, index_ref)

    def per_cell(cell, carry):
        tile_count = pack_sources(
            cell, local_cells, index_ref, entries, table_ref, lambda held: held, pack_ref.at[cell], 2
        )
        count = count_of(cell, local_cells, index_ref, columns)

        def body(span):
            xa, ya, za, ia = (spread_ref[cell, c, span, :] for c in (0, 1, 2, 6))

            def step(first, tiles, total):
                for u in range(tiles):
                    at = first + u
                    dx = xa - pack_ref[cell, at, 0:1, :]
                    dy = ya - pack_ref[cell, at, 1:2, :]
                    dz = za - pack_ref[cell, at, 2:3, :]
                    squared = dx * dx + dy * dy + dz * dz
                    scaled = squared * lax.rsqrt(jnp.maximum(squared, TINY)) * ia
                    remain = jnp.maximum(4.0 - scaled, 0.0)
                    remain = remain * remain
                    total = total + remain * remain * ((1.0 + scaled) * pack_ref[cell, at, 3:4, :])
                return total

            return step

        def finish(span, total):
            sums_ref[cell, span, :] = total

        each_group(count, tile_count, body, finish, lambda rows: jnp.zeros((rows, LANES), jnp.float32))
        return carry

    lax.fori_loop(0, local_cells, per_cell, 0)
    raw = row_sums(sums_ref, local_cells)
    masses = jnp.concatenate([table_ref[cell, 3:4, :] for cell in range(local_cells)], axis=0)
    smooth = jnp.concatenate([own_ref[cell, 10:11, :] for cell in range(local_cells)], axis=0)
    entropy = jnp.concatenate([own_ref[cell, 11:12, :] for cell in range(local_cells)], axis=0)
    held = masses > 0.0
    smooth = jnp.where(held, smooth, 1.0)
    density = jnp.where(held, raw * (kernel_norm / 256.0) / (smooth * smooth * smooth), 0.0)
    out_ref[...] = density
    bounded = jnp.where(held, density, 1.0)
    log_density = jnp.log(bounded)
    pressure_term = entropy * jnp.exp((gamma_index - 2.0) * log_density)
    sound = jnp.sqrt(gamma_index * entropy * jnp.exp((gamma_index - 1.0) * log_density))
    rows = (bounded * 0.005, pressure_term, sound * 0.025)
    for cell in range(local_cells):
        for c, row in enumerate(rows):
            state_ref[cell, c : c + 1, :] = row[cell : cell + 1]
        state_ref[cell, 3:8, :] = jnp.zeros((5, LANES), jnp.float32)
        for c in range(2):
            sent_ref[cell, c : c + 1, :] = rows[c][cell : cell + 1]
        sent_ref[cell, 2:3, :] = own_ref[cell, 8:9, :]
        sent_ref[cell, 3:4, :] = own_ref[cell, 7:8, :]


def with_sound(held):
    squared = (0.025 * 0.025 * 200.0 * gamma_index) * (held[0:1] * held[1:2])
    sound = squared * lax.rsqrt(jnp.maximum(squared, TINY))
    return jnp.concatenate([held, sound, 0.025 * held[2:3] / held[3:4]], axis=0)


def force_kernel(
    index_ref, table_ref, state_ref, pack_ref, spread_ref, state_spread_ref,
    out_ref, state_pack_ref, sums_ref, *, columns,
):
    local_cells = out_ref.shape[1]
    entries = 2 * columns + 1

    def per_cell(cell, carry):
        tile_count = pack_sources(
            cell, local_cells, index_ref, entries, state_ref, with_sound, state_pack_ref, 2
        )
        count = count_of(cell, local_cells, index_ref, columns)

        def body(span):
            def step(first, tiles, total):
                for u in range(tiles):
                    at = first + u
                    xa, ya, za, ua, va, wa = (spread_ref[cell, c, span, :] for c in range(6))
                    ga, sa, ja = (spread_ref[cell, c, span, :] for c in range(7, 10))
                    ra, fa, ca = (state_spread_ref[cell, c, span, :] for c in range(3))
                    xb, yb, zb, mb, ub, vb, wb = (pack_ref[cell, at, c : c + 1, :] for c in range(7))
                    rb, fb, sb, gb, cb, jb = (state_pack_ref[at, c : c + 1, :] for c in range(6))
                    dx, dy, dz = xa - xb, ya - yb, za - zb
                    squared = dx * dx + dy * dy + dz * dz
                    apart = squared * lax.rsqrt(jnp.maximum(squared, TINY))
                    closing = (ua - ub) * dx + (va - vb) * dy + (wa - wb) * dz
                    slope_a = jnp.maximum(sa - apart * ja, 0.0)
                    slope_a = slope_a * slope_a * slope_a
                    slope_b = jnp.maximum(sb - apart * jb, 0.0)
                    slope_b = slope_b * slope_b * slope_b
                    width = ga + gb
                    approach = jnp.minimum(width * closing, 0.0) / (squared + width * width)
                    viscous = approach * (approach - (ca + cb)) / (ra + rb)
                    coupling = ((fa + viscous) * slope_a + (fb + viscous) * slope_b) * mb
                    total = (total[0] + coupling * dx, total[1] + coupling * dy, total[2] + coupling * dz)
                return total

            return step

        def finish(span, total):
            for d in range(3):
                sums_ref[d, cell, span, :] = total[d]

        each_group(
            count, tile_count, body, finish, lambda rows: (jnp.zeros((rows, LANES), jnp.float32),) * 3
        )
        return carry

    lax.fori_loop(0, local_cells, per_cell, 0)
    held = jnp.concatenate([table_ref[cell, 3:4, :] for cell in range(local_cells)], axis=0) > 0.0
    for d in range(3):
        out_ref[d] = jnp.where(held, row_sums(sums_ref.at[d], local_cells), 0.0)


def on_chip(array):
    return pltpu.with_memory_space_constraint(array, pltpu.VMEM)


def off_chip(array):
    return pltpu.with_memory_space_constraint(array, pltpu.HBM)


def per_device(particles, counts, pair_lists):
    local_cells, _, slots = particles.shape
    columns = pair_lists.shape[1]
    assert slots == LANES and local_cells % 8 == 0
    scalars = pl.BlockSpec(memory_space=pltpu.SMEM)
    whole = pl.BlockSpec(memory_space=pltpu.VMEM)
    plain = lambda *shape: jax.ShapeDtypeStruct(shape, jnp.float32)
    floats = lambda *shape: pltpu.VMEM(shape, jnp.float32)
    particles = jnp.transpose(particles, (1, 0, 2))
    sent, padded, own = pl.pallas_call(
        prepare_kernel,
        out_shape=(plain(local_cells, 8, slots), pltpu.VMEM((local_cells, LANES), jnp.int32), floats(local_cells, 16, slots)),
        in_specs=[scalars, whole, whole],
        out_specs=(whole, whole, whole),
        name="prepare",
        compiler_params=pltpu.CompilerParams(vmem_limit_bytes=ROOM),
    )(counts, off_chip(particles), off_chip(pair_lists))

    def spread(rows, channels, after):
        return pl.pallas_call(
            spread_kernel,
            out_shape=floats(local_cells, channels, LANES, LANES),
            in_specs=[whole, pl.BlockSpec(memory_space=pl.ANY)],
            out_specs=whole,
            name="spread",
        compiler_params=pltpu.CompilerParams(vmem_limit_bytes=ROOM),
        )(rows, after)

    window, own_spread = surround(sent, lambda after: spread(own, 10, after))
    table = on_chip(window)
    most_tiles = 2 * columns + 5
    rows = table.shape[0]
    density, thermal, state, packed, index = pl.pallas_call(
        lambda *refs: density_kernel(*refs, columns=columns),
        out_shape=(
            plain(local_cells, slots),
            plain(local_cells, 4, slots),
            floats(local_cells, 8, slots),
            floats(local_cells, most_tiles, 8, LANES),
            jax.ShapeDtypeStruct((3 * local_cells, LANES), jnp.int32),
        ),
        in_specs=[whole, whole, whole, whole],
        out_specs=(whole, whole, whole, whole, scalars),
        scratch_shapes=[
            floats(local_cells, LANES, LANES),
            floats(rows, LANES),
            floats(rows, LANES),
            pltpu.VMEM((3 * local_cells, LANES), jnp.int32),
        ],
        name="density_sweep",
        compiler_params=pltpu.CompilerParams(vmem_limit_bytes=ROOM),
    )(padded, table, own, own_spread)
    states, state_spread = surround(thermal, lambda after: spread(state, 3, after))
    acceleration = pl.pallas_call(
        lambda *refs: force_kernel(*refs, columns=columns),
        out_shape=plain(3, local_cells, slots),
        in_specs=[scalars, whole, whole, whole, whole, whole],
        out_specs=whole,
        scratch_shapes=[floats(most_tiles, 6, LANES), floats(3, local_cells, LANES, LANES)],
        name="force_sweep",
        compiler_params=pltpu.CompilerParams(vmem_limit_bytes=ROOM),
    )(index, table, on_chip(states), packed, own_spread, state_spread)
    return density, jnp.transpose(acceleration, (1, 0, 2))


def solution(mesh):
    in_specs = (P(AXES, None, None), P(AXES), P(AXES, None))
    out_specs = (P(AXES, None), P(AXES, None, None))
    return jax.shard_map(per_device, mesh=mesh, in_specs=in_specs, out_specs=out_specs, check_vma=False)
```

```python
import jax
import jax.numpy as jnp
from jax import lax
from jax.experimental import pallas as pl
from jax.experimental.pallas import tpu as pltpu
from jax.sharding import PartitionSpec as P


FARTHEST = 127

gamma_index = 5.0 / 3.0
kernel_norm = 21.0 / (2.0 * 3.141592653589793)
slope_norm = 105.0 / (2.0 * 3.141592653589793)

LANES = 128
ROOM = 12 << 20
TINY = 1.2e-38
AXES = ("curve", "group")


def swap_cores(block):
    return lax.ppermute(block, "group", [(0, 1), (1, 0)])


def reach_of(local_cells):
    return -(-FARTHEST // (2 * local_cells))


def route_of(chips, k):
    route = []
    for chip in range(chips):
        route.append((2 * (chip + k) if chip + k < chips else 2 * chip + 1, 2 * chip))
        route.append((2 * (chip - k) + 1 if chip - k >= 0 else 2 * chip, 2 * chip + 1))
    return route


def surround(block, beside):
    chips = lax.axis_size("curve")
    chip_block = jnp.concatenate([block, swap_cores(block)], axis=0)
    reach = reach_of(block.shape[0])
    fetched = []
    for k in range(1, reach + 1):
        fetched.append(lax.ppermute(chip_block, AXES, route_of(chips, k)))
    made = beside(chip_block)
    fetched = jnp.concatenate(fetched, axis=0)
    return jnp.concatenate([chip_block, fetched, swap_cores(fetched)], axis=0), made


def window_starts(chip, core, local_cells, reach):
    side = 1 - 2 * core
    runs = [(chip, core), (chip, 1 - core)]
    for k in range(1, reach + 1):
        runs += [(chip + side * k, core), (chip + side * k, 1 - core)]
    for k in range(1, reach + 1):
        runs += [(chip - side * k, 1 - core), (chip - side * k, core)]
    return [((2 * where + half) * local_cells, where) for where, half in runs]


def pack_sources(cell, local_cells, index_ref, entries, table, lift, pack, pad_tiles):
    lane = lax.broadcasted_iota(jnp.int32, (1, LANES), 1)
    held = jnp.zeros(pack.shape[1:], jnp.float32)
    tile = index_ref[local_cells + cell, 0]
    for entry in range(entries):
        turn = index_ref[2 * local_cells + cell, entry]
        following = index_ref[local_cells + cell, entry + 1]
        rolled = pltpu.roll(lift(table(index_ref[cell, entry])), turn, 1)
        merged = jnp.where(lane >= turn, rolled, held)
        pack[tile] = merged
        held = jnp.where(following > tile, rolled, merged)
        tile = following
    turn = index_ref[2 * local_cells + cell, entries]
    pack[tile] = jnp.where(lane < turn, held, 0.0)
    for extra in range(1, pad_tiles):
        pack[tile + extra] = jnp.zeros(pack.shape[1:], jnp.float32)
    return jnp.where(turn > 0, tile + 1, tile)


def count_of(cell, local_cells, index_ref, entry):
    tiles = index_ref[local_cells + cell, entry + 1] - index_ref[local_cells + cell, entry]
    return 128 * tiles + index_ref[2 * local_cells + cell, entry + 1] - index_ref[2 * local_cells + cell, entry]


def each_group(most_rows, count, tile_count, body, finish, zeros):
    fours = lax.shift_right_logical(tile_count + 1, 2)
    twos = jnp.where(tile_count > 4 * fours, 1, 0)

    def per_group(start, rows):
        span = pl.ds(pl.multiple_of(start, 8), rows)
        step = body(span)
        total = zeros(rows)
        total = lax.fori_loop(0, fours, lambda k, t: step(4 * k, 4, t), total)
        total = lax.fori_loop(0, twos, lambda k, t: step(4 * fours, 2, t), total)
        finish(span, total)

    start = jnp.int32(0)
    eights = lax.shift_right_logical(count + 7, 3)
    rows = most_rows
    while rows >= 8:
        groups = lax.shift_right_logical(eights, (rows // 8).bit_length() - 1)
        groups = groups if rows == most_rows else lax.bitwise_and(groups, 1)

        def several(group, carry, start=start, rows=rows):
            per_group(start + group * rows, rows)
            return carry

        lax.fori_loop(0, groups, several, 0)
        start = start + groups * rows
        rows //= 2


def row_sums(sums, local_cells):
    lane = lax.broadcasted_iota(jnp.int32, (LANES, LANES), 1)
    held = jnp.zeros((LANES, LANES), jnp.float32)
    for cell in range(local_cells):
        held = jnp.where(lane == cell, jnp.sum(sums[cell], axis=1, keepdims=True), held)
    return jnp.transpose(held)[:local_cells]


def prepare_kernel(counts_ref, particles_ref, lists_ref, sent_ref, padded_ref, own_ref):
    local_cells, columns = lists_ref.shape
    lane = lax.broadcasted_iota(jnp.int32, (1, LANES), 1)
    padded_ref[...] = jnp.full(padded_ref.shape, -1, jnp.int32)
    padded_ref[:, 0:columns] = lists_ref[...]
    for cell in range(local_cells):
        count = counts_ref[cell]
        row = slice(cell, cell + 1)
        for c, d in enumerate((0, 1, 2, None, 3, 4, 5)):
            if d is not None:
                sent_ref[cell, c : c + 1, :] = particles_ref[d, row, :]
        sent_ref[cell, 3:4, :] = jnp.where(lane < count, particles_ref[7, row, :], 0.0)
        sent_ref[cell, 7:8, :] = ((padded_ref[row, :] + 1) * 256 + count).astype(jnp.float32)
    smooth = particles_ref[6]
    steep = slope_norm ** (1.0 / 3.0) * jnp.exp((-5.0 / 3.0) * jnp.log(smooth))
    rows = [particles_ref[d] for d in range(6)]
    rows += [2.0 / smooth, smooth * 0.05, steep, steep * (0.5 / smooth), smooth, particles_ref[8]]
    for cell in range(local_cells):
        for c, row in enumerate(rows):
            own_ref[cell, c : c + 1, :] = row[cell : cell + 1]


def spread_kernel(rows_ref, after_ref, spread_ref):
    def per_pair(pair, carry):
        cells = (2 * pair, 2 * pair + 1)
        held = [jnp.transpose(rows_ref[cell]) for cell in cells]
        for c in range(spread_ref.shape[1]):
            for cell, columns in zip(cells, held):
                spread_ref[cell, c] = jnp.broadcast_to(columns[:, c : c + 1], (LANES, LANES))
        return carry

    lax.fori_loop(0, spread_ref.shape[0] // 2, per_pair, 0)


def find_partners(padded_ref, table_ref, code_ref, ids_ref, listed_ref, found_ref, columns):
    chips = lax.axis_size("curve")
    local_cells = padded_ref.shape[0]
    reach = reach_of(local_cells)
    lane = lax.broadcasted_iota(jnp.int32, (1, LANES), 1)
    inner = lax.broadcasted_iota(jnp.int32, (8, LANES), 0)
    starts = window_starts(lax.axis_index("curve"), lax.axis_index("group"), local_cells, reach)
    groups = []
    for first in range(0, table_ref.shape[0] // 8, 8):
        start, where = starts[first // local_cells]
        span = slice(first, first + 8)
        lists = table_ref[pl.ds(8 * first + 7, 8, stride=8), :].astype(jnp.int32)
        real = (where >= 0) & (where < chips)
        count = lax.bitwise_and(lists, 255)
        code_ref[span, :] = jnp.where(real, (inner + first) * 256 + count, 0).astype(jnp.float32)
        listed_ref[span, :] = (lax.shift_right_logical(lists, 8) - 1).astype(jnp.float32)
        ids_ref[span, :] = (inner + (start + first % local_cells)).astype(jnp.float32)
        groups.append(span)
    own_start = starts[0][0]

    def per_cell(cell, carry):
        own = own_start + cell
        row = padded_ref[pl.ds(cell, 1), :]
        wanted = jnp.where(lane == columns, own, jnp.where(row >= 0, row, -(1 << 20))).astype(jnp.float32)
        own = own.astype(jnp.float32)
        ahead = jnp.zeros((8, LANES), jnp.float32)
        behind = jnp.zeros((8, LANES), jnp.float32)
        for span in groups:
            code = code_ref[span, :]
            ahead = jnp.maximum(ahead, jnp.where(ids_ref[span, :] == wanted, code, 0.0))
            behind = jnp.maximum(behind, jnp.where(listed_ref[span, :] == own, code, 0.0))
        ahead = jnp.max(ahead, axis=0, keepdims=True)
        behind = pltpu.roll(jnp.max(behind, axis=0, keepdims=True), columns + 1, 1)
        found_ref[pl.ds(cell, 1), :] = jnp.where(lane <= columns, ahead, behind).astype(jnp.int32)
        return carry

    lax.fori_loop(0, local_cells, per_cell, 0)
    code = found_ref[0:local_cells, :]
    count = lax.bitwise_and(code, 255)
    place, shift = count, 1
    while shift < 2 * columns + 1:
        place = place + jnp.where(lane >= shift, pltpu.roll(place, shift, 1), 0)
        shift *= 2
    place = place - count
    found_ref[0:local_cells, :] = lax.shift_right_logical(code, 8)
    found_ref[local_cells : 2 * local_cells, :] = lax.shift_right_logical(place, 7)
    found_ref[2 * local_cells : 3 * local_cells, :] = lax.bitwise_and(place, 127)


def density_kernel(
    padded_ref, table_ref, own_ref, spread_ref,
    out_ref, sent_ref, state_ref, pack_ref, index_ref, sums_ref, code_ref, ids_ref, listed_ref, found_ref, *, columns,
):
    local_cells = out_ref.shape[0]
    entries = 2 * columns + 1
    find_partners(padded_ref, table_ref, code_ref, ids_ref, listed_ref, found_ref, columns)
    pltpu.sync_copy(found_ref, index_ref)

    def per_cell(cell, carry):
        tile_count = pack_sources(
            cell, local_cells, index_ref, entries,
            lambda row: table_ref[pl.ds(pl.multiple_of(8 * row, 8), 8), :], lambda held: held, pack_ref.at[cell], 2,
        )
        count = count_of(cell, local_cells, index_ref, columns)

        def body(span):
            xa, ya, za, ia = (spread_ref[cell, c, span, :] for c in (0, 1, 2, 6))

            def step(first, tiles, total):
                for u in range(tiles):
                    at = first + u
                    dx = xa - pack_ref[cell, at, 0:1, :]
                    dy = ya - pack_ref[cell, at, 1:2, :]
                    dz = za - pack_ref[cell, at, 2:3, :]
                    squared = dx * dx + dy * dy + dz * dz
                    scaled = squared * lax.rsqrt(jnp.maximum(squared, TINY)) * ia
                    remain = jnp.maximum(4.0 - scaled, 0.0)
                    remain = remain * remain
                    total = total + remain * remain * ((1.0 + scaled) * pack_ref[cell, at, 3:4, :])
                return total

            return step

        def finish(span, total):
            sums_ref[cell, span, :] = total

        each_group(64, count, tile_count, body, finish, lambda rows: jnp.zeros((rows, LANES), jnp.float32))
        return carry

    lax.fori_loop(0, local_cells, per_cell, 0)
    raw = row_sums(sums_ref, local_cells)
    masses = table_ref[pl.ds(3, local_cells, stride=8), :]
    smooth = jnp.concatenate([own_ref[cell, 10:11, :] for cell in range(local_cells)], axis=0)
    entropy = jnp.concatenate([own_ref[cell, 11:12, :] for cell in range(local_cells)], axis=0)
    held = masses > 0.0
    smooth = jnp.where(held, smooth, 1.0)
    density = jnp.where(held, raw * (kernel_norm / 256.0) / (smooth * smooth * smooth), 0.0)
    out_ref[...] = density
    bounded = jnp.where(held, density, 1.0)
    log_density = jnp.log(bounded)
    pressure_term = entropy * jnp.exp((gamma_index - 2.0) * log_density)
    sound = jnp.sqrt(gamma_index * entropy * jnp.exp((gamma_index - 1.0) * log_density))
    rows = (bounded * 0.005, pressure_term, sound * 0.025)
    for cell in range(local_cells):
        for c, row in enumerate(rows):
            state_ref[cell, c : c + 1, :] = row[cell : cell + 1]
        state_ref[cell, 3:8, :] = jnp.zeros((5, LANES), jnp.float32)
        for c in range(2):
            sent_ref[cell, c : c + 1, :] = rows[c][cell : cell + 1]
        sent_ref[cell, 2:3, :] = own_ref[cell, 8:9, :]
        sent_ref[cell, 3:4, :] = own_ref[cell, 7:8, :]


def with_sound(held):
    squared = (0.025 * 0.025 * 200.0 * gamma_index) * (held[0:1] * held[1:2])
    sound = squared * lax.rsqrt(jnp.maximum(squared, TINY))
    return jnp.concatenate([held, sound, 0.025 * held[2:3] / held[3:4]], axis=0)


def force_kernel(
    index_ref, table_ref, state_ref, pack_ref, spread_ref, state_spread_ref,
    out_ref, state_pack_ref, sums_ref, *, columns,
):
    local_cells = out_ref.shape[1]
    entries = 2 * columns + 1

    def per_cell(cell, carry):
        tile_count = pack_sources(
            cell, local_cells, index_ref, entries, lambda row: state_ref[row], with_sound, state_pack_ref, 2
        )
        count = count_of(cell, local_cells, index_ref, columns)

        def body(span):
            def step(first, tiles, total):
                for u in range(tiles):
                    at = first + u
                    xa, ya, za, ua, va, wa = (spread_ref[cell, c, span, :] for c in range(6))
                    ga, sa, ja = (spread_ref[cell, c, span, :] for c in range(7, 10))
                    ra, fa, ca = (state_spread_ref[cell, c, span, :] for c in range(3))
                    xb, yb, zb, mb, ub, vb, wb = (pack_ref[cell, at, c : c + 1, :] for c in range(7))
                    rb, fb, sb, gb, cb, jb = (state_pack_ref[at, c : c + 1, :] for c in range(6))
                    dx, dy, dz = xa - xb, ya - yb, za - zb
                    squared = dx * dx + dy * dy + dz * dz
                    apart = squared * lax.rsqrt(jnp.maximum(squared, TINY))
                    closing = (ua - ub) * dx + (va - vb) * dy + (wa - wb) * dz
                    slope_a = jnp.maximum(sa - apart * ja, 0.0)
                    slope_a = slope_a * slope_a * slope_a
                    slope_b = jnp.maximum(sb - apart * jb, 0.0)
                    slope_b = slope_b * slope_b * slope_b
                    width = ga + gb
                    approach = jnp.minimum(width * closing, 0.0) / (squared + width * width)
                    viscous = approach * (approach - (ca + cb)) / (ra + rb)
                    coupling = ((fa + viscous) * slope_a + (fb + viscous) * slope_b) * mb
                    total = (total[0] + coupling * dx, total[1] + coupling * dy, total[2] + coupling * dz)
                return total

            return step

        def finish(span, total):
            for d in range(3):
                sums_ref[d, cell, span, :] = total[d]

        each_group(
            32, count, tile_count, body, finish, lambda rows: (jnp.zeros((rows, LANES), jnp.float32),) * 3
        )
        return carry

    lax.fori_loop(0, local_cells, per_cell, 0)
    held = table_ref[pl.ds(3, local_cells, stride=8), :] > 0.0
    for d in range(3):
        out_ref[d] = jnp.where(held, row_sums(sums_ref.at[d], local_cells), 0.0)


def on_chip(array):
    return pltpu.with_memory_space_constraint(array, pltpu.VMEM)


def off_chip(array):
    return pltpu.with_memory_space_constraint(array, pltpu.HBM)


def per_device(particles, counts, pair_lists):
    local_cells, _, slots = particles.shape
    columns = pair_lists.shape[1]
    assert slots == LANES and local_cells % 8 == 0
    scalars = pl.BlockSpec(memory_space=pltpu.SMEM)
    whole = pl.BlockSpec(memory_space=pltpu.VMEM)
    plain = lambda *shape: jax.ShapeDtypeStruct(shape, jnp.float32)
    floats = lambda *shape: pltpu.VMEM(shape, jnp.float32)
    particles = jnp.transpose(particles, (1, 0, 2))
    sent, padded, own = pl.pallas_call(
        prepare_kernel,
        out_shape=(plain(local_cells, 8, slots), pltpu.VMEM((local_cells, LANES), jnp.int32), floats(local_cells, 16, slots)),
        in_specs=[scalars, whole, whole],
        out_specs=(whole, whole, whole),
        name="prepare",
        compiler_params=pltpu.CompilerParams(vmem_limit_bytes=ROOM),
    )(off_chip(counts), off_chip(particles), off_chip(pair_lists))

    def spread(rows, channels, after):
        return pl.pallas_call(
            spread_kernel,
            out_shape=floats(local_cells, channels, LANES, LANES),
            in_specs=[whole, pl.BlockSpec(memory_space=pl.ANY)],
            out_specs=whole,
            name="spread",
        compiler_params=pltpu.CompilerParams(vmem_limit_bytes=ROOM),
        )(rows, after)

    window, own_spread = surround(sent, lambda after: spread(own, 10, after))
    table = on_chip(window.reshape(-1, slots))
    most_tiles = 2 * columns + 5
    rows = window.shape[0]
    density, thermal, state, packed, index = pl.pallas_call(
        lambda *refs: density_kernel(*refs, columns=columns),
        out_shape=(
            plain(local_cells, slots),
            plain(local_cells, 4, slots),
            floats(local_cells, 8, slots),
            floats(local_cells, most_tiles, 8, LANES),
            jax.ShapeDtypeStruct((3 * local_cells, LANES), jnp.int32),
        ),
        in_specs=[whole, whole, whole, whole],
        out_specs=(whole, whole, whole, whole, scalars),
        scratch_shapes=[
            floats(local_cells, LANES, LANES),
            floats(rows, LANES),
            floats(rows, LANES),
            floats(rows, LANES),
            pltpu.VMEM((3 * local_cells, LANES), jnp.int32),
        ],
        name="density_sweep",
        compiler_params=pltpu.CompilerParams(vmem_limit_bytes=ROOM),
    )(padded, table, own, own_spread)
    states, state_spread = surround(thermal, lambda after: spread(state, 3, after))
    acceleration = pl.pallas_call(
        lambda *refs: force_kernel(*refs, columns=columns),
        out_shape=plain(3, local_cells, slots),
        in_specs=[scalars, whole, whole, whole, whole, whole],
        out_specs=whole,
        scratch_shapes=[floats(most_tiles, 6, LANES), floats(3, local_cells, LANES, LANES)],
        name="force_sweep",
        compiler_params=pltpu.CompilerParams(vmem_limit_bytes=ROOM),
    )(index, table, on_chip(states), packed, own_spread, state_spread)
    return density, jnp.transpose(acceleration, (1, 0, 2))


def solution(mesh):
    in_specs = (P(AXES, None, None), P(AXES), P(AXES, None))
    out_specs = (P(AXES, None), P(AXES, None, None))
    return jax.shard_map(per_device, mesh=mesh, in_specs=in_specs, out_specs=out_specs, check_vma=False)
```
